8 devices in a mesh: dp: 1 (over z), tp: 8 (over y, x, core).
Axes of the slice: x: 2, y: 2, z: 1, core: 2. Of those that a mesh axis runs over, the one named last changes fastest.
Arguments:
- x_saved: bfloat16 [2, 1024, 4096], P('dp')
- h1_saved: bfloat16 [2, 1024, 4096], P('dp')
- grad_y: bfloat16 [2, 1024, 4096], P('dp')
- mean_one: float32 [2, 1024], P('dp')
- rstd_one: float32 [2, 1024], P('dp')
- mean_two: float32 [2, 1024], P('dp')
- rstd_two: float32 [2, 1024], P('dp')
- gain_one: bfloat16 [4096], replicated
- gain_two: bfloat16 [4096], replicated
- w_qkv: bfloat16 [4096, 32, 3, 128], P(None, 'tp')
- w_out: bfloat16 [32, 128, 4096], P('tp')
- w_up: bfloat16 [4096, 16384], P(None, 'tp')
- w_down: bfloat16 [16384, 4096], P('tp')
Outputs:
- output 1: bfloat16 [2, 1024, 4096], P('dp')
- output 2: bfloat16 [4096, 32, 3, 128], P('dp', 'tp')
- output 3: bfloat16 [32, 128, 4096], P(('dp', 'tp'))
- output 4: bfloat16 [4096, 16384], P('dp', 'tp')
- output 5: bfloat16 [16384, 4096], P(('dp', 'tp'))
All inputs are finite; a program needn't handle non-finite values.
Results may differ from the reference program's by a relative error of at most 0.0170333.
Values are sent between devices in bfloat16 or wider.
A program may use at most 1 GiB of HBM per device.

```python
import math
import jax
import jax.numpy as jnp
from jax import lax
from functools import partial

HIDDEN = 4096
NUM_HEADS = 32
FFN_DIM = 16384
SEQ_LEN = 1024
MICROBATCHES = 2

HEAD_DIM = HIDDEN // NUM_HEADS
TOKENS = MICROBATCHES * SEQ_LEN
GELU_C = 0.7978845608028654
GELU_A = 0.044715
NORM_EPS = 1e-5
wide_dot = partial(jnp.dot, preferred_element_type=jnp.float32)


def row_stats(acts):
    row_vals = acts.astype(jnp.float32)
    row_mean = jnp.mean(row_vals, axis=-1)
    row_var = jnp.mean(jnp.square(row_vals - row_mean[..., None]), axis=-1)
    return row_mean, lax.rsqrt(row_var + NORM_EPS)


def setup_inputs(seed: int = 0, part: int = 0) -> dict:
    shared_key, part_root = jax.random.split(jax.random.key(seed))
    act_keys = jax.random.split(jax.random.fold_in(part_root, part), 7)
    weight_keys = jax.random.split(shared_key, 6)
    act_shape = (MICROBATCHES, SEQ_LEN, HIDDEN)
    row_shape = (MICROBATCHES, SEQ_LEN, 1)
    x_saved = (jax.random.normal(act_keys[0], row_shape)
               + jax.random.uniform(act_keys[1], row_shape, minval=0.5, maxval=2.0)
               * jax.random.normal(act_keys[2], act_shape)).astype(jnp.bfloat16)
    h1_saved = (0.5 * jax.random.normal(act_keys[3], row_shape)
                + jax.random.uniform(act_keys[4], row_shape, minval=0.4, maxval=1.2)
                * jax.random.normal(act_keys[5], act_shape)).astype(jnp.bfloat16)
    grad_y = jax.random.normal(act_keys[6], act_shape).astype(jnp.bfloat16)
    mean_one, rstd_one = row_stats(x_saved)
    mean_two, rstd_two = row_stats(h1_saved)
    gain_one = jax.random.uniform(weight_keys[0], (HIDDEN,), minval=0.5, maxval=1.5).astype(jnp.bfloat16)
    gain_two = jax.random.uniform(weight_keys[1], (HIDDEN,), minval=0.5, maxval=1.5).astype(jnp.bfloat16)
    qk_gain = math.sqrt(math.log(SEQ_LEN))
    head_gain = jnp.array([qk_gain, 1.0, 1.0], dtype=jnp.float32)[:, None]
    w_qkv = (jax.random.normal(weight_keys[2], (HIDDEN, NUM_HEADS, 3, HEAD_DIM)) * head_gain
             * HIDDEN ** -0.5).astype(jnp.bfloat16)
    w_out = (jax.random.normal(weight_keys[3], (NUM_HEADS, HEAD_DIM, HIDDEN)) * HIDDEN ** -0.5).astype(jnp.bfloat16)
    w_up = (jax.random.normal(weight_keys[4], (HIDDEN, FFN_DIM)) * HIDDEN ** -0.5).astype(jnp.bfloat16)
    w_down = (jax.random.normal(weight_keys[5], (FFN_DIM, HIDDEN)) * FFN_DIM ** -0.5).astype(jnp.bfloat16)
    return {'x_saved': x_saved, 'h1_saved': h1_saved, 'grad_y': grad_y,
            'mean_one': mean_one, 'rstd_one': rstd_one, 'mean_two': mean_two, 'rstd_two': rstd_two,
            'gain_one': gain_one, 'gain_two': gain_two,
            'w_qkv': w_qkv, 'w_out': w_out, 'w_up': w_up, 'w_down': w_down}


def gelu_tanh(pre_act):
    inner_arg = GELU_C * (pre_act + GELU_A * pre_act * pre_act * pre_act)
    return 0.5 * pre_act * (1.0 + jnp.tanh(inner_arg))


def gelu_slope(pre_act):
    inner_arg = GELU_C * (pre_act + GELU_A * pre_act * pre_act * pre_act)
    tanh_val = jnp.tanh(inner_arg)
    return (0.5 * (1.0 + tanh_val)
            + 0.5 * pre_act * (1.0 - tanh_val * tanh_val) * GELU_C * (1.0 + 3.0 * GELU_A * pre_act * pre_act))


def norm_backward(grad_norm, xhat, gain, rstd):
    scaled = grad_norm * gain.astype(jnp.float32)
    mean_scaled = jnp.mean(scaled, axis=-1, keepdims=True)
    mean_cross = jnp.mean(scaled * xhat, axis=-1, keepdims=True)
    return rstd[..., None] * (scaled - mean_scaled - xhat * mean_cross)


def head_backward(operands):
    q_heads, k_heads, v_heads, grad_o = operands
    score_scale = HEAD_DIM ** -0.5
    scores = wide_dot(q_heads, k_heads.T) * score_scale
    causal = jnp.arange(SEQ_LEN)[:, None] >= jnp.arange(SEQ_LEN)[None, :]
    attn_prob = jax.nn.softmax(jnp.where(causal, scores, -1e30), axis=-1)
    prob_bf16 = attn_prob.astype(jnp.bfloat16)
    attn_out = wide_dot(prob_bf16, v_heads).astype(jnp.bfloat16)
    grad_v = wide_dot(prob_bf16.T, grad_o).astype(jnp.bfloat16)
    grad_p = wide_dot(grad_o, v_heads.T)
    row_dot = jnp.sum(attn_prob * grad_p, axis=-1, keepdims=True)
    grad_s = (attn_prob * (grad_p - row_dot) * score_scale).astype(jnp.bfloat16)
    grad_q = wide_dot(grad_s, k_heads).astype(jnp.bfloat16)
    grad_k = wide_dot(grad_s.T, q_heads).astype(jnp.bfloat16)
    return attn_out, jnp.stack([grad_q, grad_k, grad_v], axis=1)


def split_heads(rows):
    return rows.reshape(MICROBATCHES, SEQ_LEN, NUM_HEADS, HEAD_DIM).transpose(0, 2, 1, 3).reshape(
        MICROBATCHES * NUM_HEADS, SEQ_LEN, HEAD_DIM)


def reference(x_saved, h1_saved, grad_y, mean_one, rstd_one, mean_two, rstd_two,
              gain_one, gain_two, w_qkv, w_out, w_up, w_down):
    x_rows = x_saved.reshape(TOKENS, HIDDEN)
    h1_rows = h1_saved.reshape(TOKENS, HIDDEN)
    dy_rows = grad_y.reshape(TOKENS, HIDDEN)
    xhat_two = (h1_rows.astype(jnp.float32) - mean_two.reshape(TOKENS, 1)) * rstd_two.reshape(TOKENS, 1)
    norm_two = (xhat_two * gain_two.astype(jnp.float32)).astype(jnp.bfloat16)
    pre_act = wide_dot(norm_two, w_up)
    act_out = gelu_tanh(pre_act).astype(jnp.bfloat16)
    grad_down = wide_dot(act_out.T, dy_rows).astype(jnp.bfloat16)
    grad_pre = (wide_dot(dy_rows, w_down.T) * gelu_slope(pre_act)).astype(jnp.bfloat16)
    grad_up = wide_dot(norm_two.T, grad_pre).astype(jnp.bfloat16)
    grad_norm_two = wide_dot(grad_pre, w_up.T)
    grad_h1 = (dy_rows.astype(jnp.float32)
               + norm_backward(grad_norm_two, xhat_two, gain_two, rstd_two.reshape(TOKENS))).astype(jnp.bfloat16)
    xhat_one = (x_rows.astype(jnp.float32) - mean_one.reshape(TOKENS, 1)) * rstd_one.reshape(TOKENS, 1)
    norm_one = (xhat_one * gain_one.astype(jnp.float32)).astype(jnp.bfloat16)
    qkv_flat = w_qkv.reshape(HIDDEN, 3 * HIDDEN)
    qkv_acts = wide_dot(norm_one, qkv_flat).astype(jnp.bfloat16).reshape(TOKENS, NUM_HEADS, 3, HEAD_DIM)
    grad_o = wide_dot(grad_h1, w_out.reshape(HIDDEN, HIDDEN).T).astype(jnp.bfloat16)
    attn_heads, grad_heads = lax.map(head_backward, (split_heads(qkv_acts[:, :, 0]), split_heads(qkv_acts[:, :, 1]),
                                                     split_heads(qkv_acts[:, :, 2]), split_heads(grad_o)))
    attn_rows = attn_heads.reshape(MICROBATCHES, NUM_HEADS, SEQ_LEN, HEAD_DIM).transpose(0, 2, 1, 3).reshape(
        TOKENS, HIDDEN)
    grad_qkv = grad_heads.reshape(MICROBATCHES, NUM_HEADS, SEQ_LEN, 3, HEAD_DIM).transpose(0, 2, 1, 3, 4).reshape(
        TOKENS, 3 * HIDDEN)
    grad_out_w = wide_dot(attn_rows.T, grad_h1).astype(jnp.bfloat16).reshape(NUM_HEADS, HEAD_DIM, HIDDEN)
    grad_qkv_w = wide_dot(norm_one.T, grad_qkv).astype(jnp.bfloat16).reshape(HIDDEN, NUM_HEADS, 3, HEAD_DIM)
    grad_norm_one = wide_dot(grad_qkv, qkv_flat.T)
    grad_x = (grad_h1.astype(jnp.float32)
              + norm_backward(grad_norm_one, xhat_one, gain_one, rstd_one.reshape(TOKENS))).astype(jnp.bfloat16)
    return grad_x.reshape(MICROBATCHES, SEQ_LEN, HIDDEN), grad_qkv_w, grad_out_w, grad_up, grad_down
```

```python
import jax
import jax.numpy as jnp
from jax import lax
from jax.sharding import PartitionSpec as P
from jax.experimental import pallas as pl
from jax.experimental.pallas import tpu as pltpu
from functools import partial

GELU_C = 0.7978845608028654
GELU_A = 0.044715
F32 = jnp.float32
BF16 = jnp.bfloat16
BQ = 256
NT = (((1,), (1,)), ((), ()))
TN = (((0,), (0,)), ((), ()))
ANY = pl.BlockSpec(memory_space=pl.ANY)
TOKEN = jax.ShapeDtypeStruct((8, 128), F32)


def mm(a, b, dims=(((1,), (0,)), ((), ()))):
    return lax.dot_general(a, b, dims, preferred_element_type=F32)


def call(body, grid, in_specs, args, out_specs, outs, token, flops, scratch=(), pos=None, name=None):
    n_in, n_out, n_pos = len(args), len(outs), 0 if pos is None else 1

    def kernel(*refs):
        head, refs = refs[:n_pos], refs[n_pos:]
        body(*head, *refs[:n_in], *refs[n_in + 1:n_in + 1 + n_out], *refs[n_in + 2 + n_out:])

    size = sum(o.size * o.dtype.itemsize for o in outs) + sum(a.size * a.dtype.itemsize for a in args)
    results = pl.pallas_call(
        kernel,
        grid_spec=pltpu.PrefetchScalarGridSpec(
            num_scalar_prefetch=n_pos, grid=grid, in_specs=list(in_specs) + [ANY],
            out_specs=list(out_specs) + [ANY], scratch_shapes=list(scratch)),
        out_shape=list(outs) + [TOKEN],
        compiler_params=pltpu.CompilerParams(vmem_limit_bytes=60 * 1024 * 1024),
        cost_estimate=pl.CostEstimate(flops=int(flops), bytes_accessed=int(size), transcendentals=0),
        name=name,
    )(*([] if pos is None else [pos]), *args, token)
    return results


def sds(shape, dtype=BF16):
    return jax.ShapeDtypeStruct(shape, dtype)


def normed(rows, stats, gain):
    return ((rows.astype(F32) - stats[:, 0:1]) * stats[:, 1:2] * gain.astype(F32)).astype(BF16)


def mlp_kernel(h_ref, dy_ref, st_ref, g_ref, up_ref, down_ref, n_ref, act_ref, dpre_ref):
    @pl.when(pl.program_id(1) == 0)
    def _():
        n_ref[...] = normed(h_ref[0], st_ref[0], g_ref[...])

    for j in range(up_ref.shape[1] // 256):
        cols = pl.ds(j * 256, 256)
        a = mm(n_ref[...], up_ref[:, cols])
        b = mm(dy_ref[0], down_ref[cols, :], NT)
        tanh = jnp.tanh(GELU_C * (a + GELU_A * a * a * a))
        act_ref[:, cols] = (0.5 * a * (1.0 + tanh)).astype(BF16)
        slope = (0.5 * (1.0 + tanh)
                 + 0.5 * a * (1.0 - tanh * tanh) * GELU_C * (1.0 + 3.0 * GELU_A * a * a))
        dpre_ref[:, cols] = (b * slope).astype(BF16)


def mlp(m, h1, dy, stats, gain, w_up, w_down, token):
    _, seq, hid = h1.shape
    ffn = w_up.shape[1]
    bm, bn = 512, 512
    row = pl.BlockSpec((1, bm, hid), lambda i, j: (m, i, 0))
    tile = pl.BlockSpec((bm, bn), lambda i, j: (i, j))
    return call(
        mlp_kernel, (seq // bm, ffn // bn),
        [row, row, pl.BlockSpec((1, bm, 2), lambda i, j: (m, i, 0)), pl.BlockSpec((1, hid), lambda i, j: (0, 0)),
         pl.BlockSpec((hid, bn), lambda i, j: (0, j)), pl.BlockSpec((bn, hid), lambda i, j: (j, 0))],
        [h1, dy, stats, gain, w_up, w_down],
        [pl.BlockSpec((bm, hid), lambda i, j: (i, 0)), tile, tile],
        [sds((seq, hid)), sds((seq, ffn)), sds((seq, ffn))], token, 4 * seq * hid * ffn, name='mlp')


def qkv_kernel(x_ref, st_ref, g_ref, w_ref, n_ref, out_ref):
    @pl.when(pl.program_id(1) == 0)
    def _():
        n_ref[...] = normed(x_ref[0], st_ref[0], g_ref[...])

    out_ref[...] = mm(n_ref[...], w_ref[...]).astype(BF16)


def qkv_proj(m, x, stats, gain, w, token):
    _, seq, hid = x.shape
    bm, bn = 512, 512
    return call(
        qkv_kernel, (seq // bm, w.shape[1] // bn),
        [pl.BlockSpec((1, bm, hid), lambda i, j: (m, i, 0)), pl.BlockSpec((1, bm, 2), lambda i, j: (m, i, 0)),
         pl.BlockSpec((1, hid), lambda i, j: (0, 0)), pl.BlockSpec((hid, bn), lambda i, j: (0, j))],
        [x, stats, gain, w],
        [pl.BlockSpec((bm, hid), lambda i, j: (i, 0)), pl.BlockSpec((bm, bn), lambda i, j: (i, j))],
        [sds((seq, hid)), sds((seq, w.shape[1]))], token, 2 * seq * hid * w.shape[1], name='qkv')


def part_kernel(own, n_lhs, pos_ref, *refs):
    lhs, w_ref, rest = refs[:n_lhs], refs[n_lhs], refs[n_lhs + 1:]
    rows_ref = rest[-1]
    chip, core = pos_ref[1], pos_ref[2]
    blk = rows_ref.shape[0] // 4

    @pl.when(pl.program_id(0) == 0)
    def _():
        for k in range(4):
            start = (2 * jnp.bitwise_xor(chip, k) + (core if own else 1 - core)) * blk
            at = 0
            for ref in lhs:
                rows_ref[pl.ds(k * blk, blk), pl.ds(at, ref.shape[1])] = ref[pl.ds(start, blk), :]
                at += ref.shape[1]

    prod = mm(rows_ref[...], w_ref[...], NT)
    if own:
        got_ref, keep_ref = rest[0], rest[1]
        prod = prod + got_ref[...].astype(F32)
        keep_ref[...] = prod[:blk]
        for k in range(1, 4):
            rest[1 + k][...] = prod[k * blk:(k + 1) * blk].astype(BF16)
    else:
        rest[0][...] = prod.astype(BF16)


def partial_product(own, lhs, w, got, pos, token):
    seq = lhs[0].shape[0]
    hid, depth = w.shape
    bn, blk = 512, seq // 8
    in_specs = [pl.BlockSpec(l.shape, lambda j, p: (0, 0)) for l in lhs] + [pl.BlockSpec((bn, depth), lambda j, p: (j, 0))]
    args = list(lhs) + [w]
    if own:
        in_specs.append(pl.BlockSpec((4 * blk, bn), lambda j, p: (0, j)))
        args.append(got)
        out_specs = [pl.BlockSpec((blk, bn), lambda j, p: (0, j))] * 4
        outs = [sds((blk, hid), F32)] + [sds((blk, hid))] * 3
    else:
        out_specs = [pl.BlockSpec((4 * blk, bn), lambda j, p: (0, j))]
        outs = [sds((4 * blk, hid))]
    return call(partial(part_kernel, own, len(lhs)), (hid // bn,), in_specs, args, out_specs, outs, token,
                2 * seq // 2 * hid * depth, scratch=[pltpu.VMEM((4 * blk, depth), BF16)], pos=pos,
                name='own' if own else 'other')


def norm_kernel(pos_ref, keep_ref, r1_ref, r2_ref, r3_ref, act_ref, res_ref, st_ref, g_ref, out_ref):
    total = keep_ref[...] + r1_ref[...].astype(F32) + r2_ref[...].astype(F32) + r3_ref[...].astype(F32)
    rstd = st_ref[0, :, 1:2]
    hat = (act_ref[0].astype(F32) - st_ref[0, :, 0:1]) * rstd
    scaled = total * g_ref[...].astype(F32)
    mean_scaled = jnp.mean(scaled, axis=-1, keepdims=True)
    mean_cross = jnp.mean(scaled * hat, axis=-1, keepdims=True)
    res = res_ref[...].reshape(hat.shape).astype(F32)
    out_ref[...] = (res + rstd * (scaled - mean_scaled - hat * mean_cross)).astype(BF16)


def norm_shard(m, keep, got, acts, resid, stats, gain, pos, token):
    blk, hid = keep.shape
    bm = 32
    n = blk // bm
    local = pl.BlockSpec((bm, hid), lambda i, p: (i, 0))
    row = pl.BlockSpec((1, bm, hid), lambda i, p: (m, p[0] * n + i, 0))
    return call(
        norm_kernel, (n,),
        [local] * 4 + [row, row if resid.ndim == 3 else local,
                       pl.BlockSpec((1, bm, 2), lambda i, p: (m, p[0] * n + i, 0)), pl.BlockSpec((1, hid), lambda i, p: (0, 0))],
        [keep, *got, acts, resid, stats, gain], [local], [sds((blk, hid))], token, 20 * blk * hid, pos=pos, name='norm')


def proj_kernel(x_ref, w_ref, out_ref):
    out_ref[...] = mm(x_ref[...], w_ref[...], NT).astype(BF16)


def out_proj(dh, w, token):
    seq, hid = dh.shape
    bm = 256
    return call(proj_kernel, (seq // bm,),
                [pl.BlockSpec((bm, hid), lambda i: (i, 0)), pl.BlockSpec(w.shape, lambda i: (0, 0))], [dh, w],
                [pl.BlockSpec((bm, w.shape[0]), lambda i: (i, 0))], [sds((seq, w.shape[0]))], token,
                2 * seq * hid * w.shape[0], name='dout')


def attn_kernel(scale, q_ref, k_ref, v_ref, do_ref, o_ref, dq_ref, dk_ref, dv_ref, dk_acc, dv_acc):
    seq, dim = do_ref.shape
    k_all, v_all = k_ref[...], v_ref[...]
    k_t, v_t = k_all.T, v_all.T
    nblk = seq // BQ
    for i in reversed(range(nblk)):
        rows = pl.ds(i * BQ, BQ)
        width = (i + 1) * BQ
        q, do = q_ref[rows, :], do_ref[rows, :]
        s_t = mm(k_all[:width], q, NT) * scale
        kpos = lax.broadcasted_iota(jnp.int32, (width, BQ), 0)
        qpos = lax.broadcasted_iota(jnp.int32, (width, BQ), 1) + i * BQ
        s_t = jnp.where(qpos >= kpos, s_t, -1e30)
        top = jnp.max(s_t, axis=0, keepdims=True)
        p_t = jnp.exp(s_t - top)
        p_t = p_t * (1.0 / jnp.sum(p_t, axis=0, keepdims=True))
        p_b = p_t.astype(BF16)
        o_ref[rows, :] = mm(v_t[:, :width], p_b).T.astype(BF16)
        dp_t = mm(v_all[:width], do, NT)
        dot = jnp.sum(p_t * dp_t, axis=0, keepdims=True)
        ds_t = (p_t * (dp_t - dot) * scale).astype(BF16)
        dq_ref[rows, :] = mm(k_t[:, :width], ds_t).T.astype(BF16)
        dv, dk = mm(p_b, do), mm(ds_t, q)
        if i == nblk - 1:
            dv_acc[...] = dv
            dk_acc[...] = dk
        else:
            dv_acc[:width] += dv
            dk_acc[:width] += dk
    dk_ref[...] = dk_acc[...].astype(BF16)
    dv_ref[...] = dv_acc[...].astype(BF16)


def attention(qkv, do, dim, scale, token):
    seq, width = do.shape
    n = width // dim
    head = lambda c: pl.BlockSpec((seq, dim), lambda i: (0, c * n + i))
    return call(partial(attn_kernel, scale), (n,), [head(0), head(1), head(2), head(0)], [qkv, qkv, qkv, do],
                [head(0)] * 4, [sds((seq, width))] * 4, token, 24 * n * seq * seq * dim,
                scratch=[pltpu.VMEM((seq, dim), F32)] * 2, name='attn')


def grad_kernel(a0_ref, a1_ref, b0_ref, b1_ref, out_ref):
    left = lambda ref: ref[0] if len(ref.shape) == 3 else ref[...]
    acc = mm(left(a0_ref), left(b0_ref), TN) + mm(left(a1_ref), left(b1_ref), TN)
    out_ref[...] = acc.astype(BF16)


def weight_grad(lhs, rhs, token, ba, bb, name):
    def split(v, size, axis):
        if isinstance(v, (list, tuple)):
            spec = pl.BlockSpec((v[0].shape[0], size), lambda i, j: (0, (i, j)[axis]))
            return list(v), [spec] * 2, v[0].shape
        specs = [pl.BlockSpec((1, v.shape[1], size), lambda i, j, m=m: (m, 0, (i, j)[axis])) for m in range(2)]
        return [v, v], specs, v.shape[1:]

    la, ls, (seq, wa) = split(lhs, ba, 0)
    ra, rs, (_, wb) = split(rhs, bb, 1)
    return call(grad_kernel, (wa // ba, wb // bb), ls + rs, la + ra, [pl.BlockSpec((ba, bb), lambda i, j: (i, j))],
                [sds((wa, wb))], token, 4 * seq * wa * wb, name=name)


def qkv_grad_kernel(a0_ref, a1_ref, *refs):
    out_ref = refs[-1]
    rows, _, heads, dim = out_ref.shape
    for c in range(3):
        acc = mm(a0_ref[...], refs[c][...], TN) + mm(a1_ref[...], refs[3 + c][...], TN)
        out_ref[:, c] = acc.reshape(rows, heads, dim).astype(BF16)


def qkv_grad(norms, grads, heads, dim, token):
    seq, hid = norms[0].shape
    ba = 256
    lhs = pl.BlockSpec((seq, ba), lambda i: (0, i))
    whole = pl.BlockSpec((seq, heads * dim), lambda i: (0, 0))
    return call(qkv_grad_kernel, (hid // ba,), [lhs] * 2 + [whole] * 6, [*norms, *grads[0], *grads[1]],
                [pl.BlockSpec((ba, 3, heads, dim), lambda i: (i, 0, 0, 0))], [sds((hid, 3, heads, dim))], token,
                12 * seq * hid * heads * dim, name='dqkvw')


def flat_kernel(w_ref, out_ref):
    rows, _, heads, dim = w_ref.shape
    for c in range(3):
        out_ref[:, pl.ds(c * heads * dim, heads * dim)] = w_ref[:, c].reshape(rows, heads * dim)


def flat_weight(w, token):
    hid, three, heads, dim = w.shape
    bm = 256
    return call(flat_kernel, (hid // bm,), [pl.BlockSpec((bm, three, heads, dim), lambda i: (i, 0, 0, 0))], [w],
                [pl.BlockSpec((bm, three * heads * dim), lambda i: (i, 0))], [sds((hid, three * heads * dim))], token,
                w.size, name='flat')


def swap(arr, bit):
    return lax.ppermute(arr, 'tp', [(i, i ^ bit) for i in range(8)])


def solution(mesh):
    act_spec = P('dp', None, None)
    stat_spec = P('dp', None)
    in_specs = (act_spec, act_spec, act_spec, stat_spec, stat_spec, stat_spec, stat_spec, P(), P(),
                P(None, 'tp', None, None), P('tp', None, None), P(None, 'tp'), P('tp', None))
    out_specs = (act_spec, P('dp', 'tp', None, None), P(('dp', 'tp'), None, None), P('dp', 'tp'),
                 P(('dp', 'tp'), None))

    def local_backward(x_saved, h1_saved, grad_y, mean_one, rstd_one, mean_two, rstd_two,
                       gain_one, gain_two, w_qkv, w_out, w_up, w_down):
        hid, heads, _, dim = w_qkv.shape
        scale = dim ** -0.5
        idx = lax.axis_index('tp')
        pos = jnp.stack([idx, idx // 2, idx % 2]).astype(jnp.int32)
        stats_one = jnp.stack([mean_one, rstd_one], axis=-1)
        stats_two = jnp.stack([mean_two, rstd_two], axis=-1)
        g1, g2 = gain_one.reshape(1, hid), gain_two.reshape(1, hid)
        w_out = w_out.reshape(heads * dim, hid)
        tok = jnp.zeros((8, 128), F32)

        def gather(shard):
            return lax.all_gather(shard, 'tp', axis=0, tiled=True)

        def exchange(sends):
            return [swap(s, bit) for s, bit in zip(sends, (2, 4, 6))]

        w_flat, tok = flat_weight(w_qkv.transpose(0, 2, 1, 3), tok)
        n2, act, dpre, n1, qkv = [0, 0], [0, 0], [0, 0], [0, 0], [0, 0]
        dh_shard, dh, out, grads, dx = [0, 0], [0, 0], [0, 0], [0, 0], [0, 0]

        n2[0], act[0], dpre[0], tok = mlp(0, h1_saved, grad_y, stats_two, g2, w_up, w_down, tok)
        send, tok = partial_product(False, [dpre[0]], w_up, None, pos, tok)
        got = swap(send, 1)
        n1[0], qkv[0], tok = qkv_proj(0, x_saved, stats_one, g1, w_flat, tok)
        keep_a, *send, tok = partial_product(True, [dpre[0]], w_up, got, pos, tok)
        got_a = exchange(send)
        n2[1], act[1], dpre[1], tok = mlp(1, h1_saved, grad_y, stats_two, g2, w_up, w_down, tok)
        send, tok = partial_product(False, [dpre[1]], w_up, None, pos, tok)
        got = swap(send, 1)
        dh_shard[0], tok = norm_shard(0, keep_a, got_a, h1_saved, grad_y, stats_two, g2, pos, tok)
        dh[0] = gather(dh_shard[0])
        n1[1], qkv[1], tok = qkv_proj(1, x_saved, stats_one, g1, w_flat, tok)
        keep_b, *send, tok = partial_product(True, [dpre[1]], w_up, got, pos, tok)
        got_b = exchange(send)
        grad_down, tok = weight_grad(act, grad_y, tok, 512, 1024, 'dw2')
        grad_o, tok = out_proj(dh[0], w_out, tok)
        out[0], *grads[0], tok = attention(qkv[0], grad_o, dim, scale, tok)
        send, tok = partial_product(False, grads[0], w_flat, None, pos, tok)
        got = swap(send, 1)
        dh_shard[1], tok = norm_shard(1, keep_b, got_b, h1_saved, grad_y, stats_two, g2, pos, tok)
        dh[1] = gather(dh_shard[1])
        keep_a, *send, tok = partial_product(True, grads[0], w_flat, got, pos, tok)
        got_a = exchange(send)
        grad_up, tok = weight_grad(n2, dpre, tok, 512, 1024, 'dw1')
        grad_o, tok = out_proj(dh[1], w_out, tok)
        out[1], *grads[1], tok = attention(qkv[1], grad_o, dim, scale, tok)
        send, tok = partial_product(False, grads[1], w_flat, None, pos, tok)
        got = swap(send, 1)
        dx_shard, tok = norm_shard(0, keep_a, got_a, x_saved, dh_shard[0], stats_one, g1, pos, tok)
        dx[0] = gather(dx_shard)
        keep_b, *send, tok = partial_product(True, grads[1], w_flat, got, pos, tok)
        got_b = exchange(send)
        grad_qkv_w, tok = qkv_grad(n1, grads, heads, dim, tok)
        dx_shard, tok = norm_shard(1, keep_b, got_b, x_saved, dh_shard[1], stats_one, g1, pos, tok)
        dx[1] = gather(dx_shard)
        grad_out_w, tok = weight_grad(out, dh, tok, 512, 512, 'dwo')
        return (jnp.stack(dx), grad_qkv_w.transpose(0, 2, 1, 3), grad_out_w.reshape(heads, dim, hid), grad_up, grad_down)

    return jax.shard_map(local_backward, mesh=mesh, in_specs=in_specs, out_specs=out_specs, check_vma=False)
```

```python
import jax
import jax.numpy as jnp
from jax import lax
from jax.sharding import PartitionSpec as P
from jax.experimental import pallas as pl
from jax.experimental.pallas import tpu as pltpu
from functools import partial

GELU_C = 0.7978845608028654
GELU_A = 0.044715
F32 = jnp.float32
BF16 = jnp.bfloat16
BQ = 256
NT = (((1,), (1,)), ((), ()))
TN = (((0,), (0,)), ((), ()))
ANY = pl.BlockSpec(memory_space=pl.ANY)
TOKEN = jax.ShapeDtypeStruct((8, 128), F32)


def mm(a, b, dims=(((1,), (0,)), ((), ()))):
    return lax.dot_general(a, b, dims, preferred_element_type=F32)


def call(body, grid, in_specs, args, out_specs, outs, token, flops, scratch=(), pos=None, name=None, alias=None, cid=None):
    n_in, n_out, n_pos = len(args), len(outs), 0 if pos is None else 1

    def kernel(*refs):
        head, refs = refs[:n_pos], refs[n_pos:]
        body(*head, *refs[:n_in], *refs[n_in + 1:n_in + 1 + n_out], *refs[n_in + 2 + n_out:])

    size = sum(o.size * o.dtype.itemsize for o in outs) + sum(a.size * a.dtype.itemsize for a in args)
    results = pl.pallas_call(
        kernel,
        grid_spec=pltpu.PrefetchScalarGridSpec(
            num_scalar_prefetch=n_pos, grid=grid, in_specs=list(in_specs) + [ANY],
            out_specs=list(out_specs) + [ANY], scratch_shapes=list(scratch)),
        out_shape=list(outs) + [TOKEN],
        compiler_params=pltpu.CompilerParams(vmem_limit_bytes=62 * 1024 * 1024, collective_id=cid, has_side_effects=cid is not None),
        cost_estimate=pl.CostEstimate(flops=int(flops), bytes_accessed=int(size), transcendentals=0),
        input_output_aliases=alias or {},
        name=name,
    )(*([] if pos is None else [pos]), *args, token)
    return results


def sds(shape, dtype=BF16):
    return jax.ShapeDtypeStruct(shape, dtype)


def normed(rows, stats, gain):
    return ((rows.astype(F32) - stats[:, 0:1]) * stats[:, 1:2] * gain.astype(F32)).astype(BF16)


class Split:
    def __init__(self, lhs, w_hbm, outs, wrow, prod, got, w_sem, send_sem, recv_sem):
        self.lhs, self.w_hbm, self.outs = lhs, w_hbm, outs
        self.wrow, self.prod, self.got = wrow, prod, got
        self.w_sem, self.send_sem, self.recv_sem = w_sem, send_sem, recv_sem
        self.wide = wrow.shape[1]
        self.tiles = w_hbm.shape[0] // self.wide
        self.blk = prod.shape[1] // 8
        idx = lax.axis_index('tp')
        self.chip, self.core = lax.div(idx, 2), lax.rem(idx, 2)
        self.partner = 2 * self.chip + 1 - self.core

    def load(self, t):
        return pltpu.make_async_copy(self.w_hbm.at[pl.ds(t * self.wide, self.wide), :], self.wrow.at[t % 2],
                                     self.w_sem.at[t % 2])

    def rows(self, k, core):
        return pl.ds(pl.multiple_of((2 * lax.bitwise_xor(self.chip, k) + core) * self.blk, self.blk), self.blk)

    def send(self, t, k):
        return pltpu.make_async_remote_copy(
            src_ref=self.prod.at[t % 2, self.rows(k, 1 - self.core)], dst_ref=self.got.at[t, k],
            send_sem=self.send_sem.at[t, k], recv_sem=self.recv_sem.at[t, k],
            device_id={'tp': self.partner}, device_id_type=pl.DeviceIdType.MESH)

    def greet(self):
        barrier = pltpu.get_barrier_semaphore()
        pl.semaphore_signal(barrier, inc=1, device_id={'tp': self.partner}, device_id_type=pl.DeviceIdType.MESH)
        pl.semaphore_wait(barrier, 1)

    def tile(self, t):
        @pl.when(t < self.tiles)
        def _():
            self.load(t).wait()

            @pl.when(t >= 2)
            def _():
                for k in range(4):
                    self.send(t - 2, k).wait_send()

            self.prod[t % 2] = mm(self.lhs[...], self.wrow[t % 2], NT).astype(BF16)
            for k in range(4):
                self.send(t, k).start()

            @pl.when(t + 2 < self.tiles)
            def _():
                self.load(t + 2).start()

        @pl.when(t > 0)
        def _():
            for k in range(4):
                self.send(t - 1, k).wait_recv()
                total = self.prod[(t - 1) % 2, self.rows(k, self.core)].astype(F32) + self.got[t - 1, k].astype(F32)
                self.outs[k][...] = total.astype(self.outs[k].dtype)

        @pl.when(t == self.tiles)
        def _():
            for u in range(self.tiles - 2, self.tiles):
                for k in range(4):
                    self.send(u, k).wait_send()

    @staticmethod
    def scratch(seq, depth, hid, wide):
        tiles = hid // wide
        return [pltpu.VMEM((2, wide, depth), BF16), pltpu.VMEM((2, seq, wide), BF16),
                pltpu.VMEM((tiles, 4, seq // 8, wide), BF16), pltpu.SemaphoreType.DMA((2,)),
                pltpu.SemaphoreType.DMA((tiles, 4)), pltpu.SemaphoreType.DMA((tiles, 4))]

    @staticmethod
    def out(seq, hid, wide, first):
        last = hid // wide - 1
        spec = pl.BlockSpec((seq // 8, wide), lambda j: (0, jnp.clip(j - first - 1, 0, last)))
        return [spec] * 4, [sds((seq // 8, hid), F32)] + [sds((seq // 8, hid))] * 3


def gelu_pair(a, b):
    tanh = jnp.tanh(GELU_C * (a + GELU_A * a * a * a))
    slope = (0.5 * (1.0 + tanh)
             + 0.5 * a * (1.0 - tanh * tanh) * GELU_C * (1.0 + 3.0 * GELU_A * a * a))
    return (0.5 * a * (1.0 + tanh)).astype(BF16), (b * slope).astype(BF16)


def mlp_kernel(m, nt, h_ref, dy_ref, st_ref, g_ref, up_ref, down_ref, up_hbm,
               n_hbm, act_ref, dpre_hbm, keep_ref, s1_ref, s2_ref, s3_ref,
               n_v, dy_v, dpre_v, h_sem, dy_sem, out_sem, *split_refs):
    step = pl.program_id(0)
    bn = up_ref.shape[1]
    chunks = h_sem.shape[0]
    part = n_v.shape[0] // chunks
    split = Split(dpre_v, up_hbm, (keep_ref, s1_ref, s2_ref, s3_ref), *split_refs)
    n_out = pltpu.make_async_copy(n_v, n_hbm, out_sem.at[0])
    d_out = pltpu.make_async_copy(dpre_v, dpre_hbm, out_sem.at[1])

    def load(r):
        rows = pl.ds(pl.multiple_of(r * part, part), part)
        return (pltpu.make_async_copy(h_ref.at[m, rows], n_v.at[rows], h_sem.at[r]),
                pltpu.make_async_copy(dy_ref.at[m, rows], dy_v.at[rows], dy_sem.at[r]))

    @pl.when(step == 0)
    def _():
        for r in range(chunks):
            for copy in load(r):
                copy.start()
        split.greet()

        @pl.loop(0, chunks)
        def _(r):
            rows = pl.ds(pl.multiple_of(r * part, part), part)
            h_copy, dy_copy = load(r)
            h_copy.wait()
            n_v[rows, :] = normed(n_v[rows, :], st_ref[0, rows, :], g_ref[...])
            dy_copy.wait()
            act, dpre = gelu_pair(mm(n_v[rows, :], up_ref[...]), mm(dy_v[rows, :], down_ref[...], NT))
            act_ref[rows, :] = act
            dpre_v[rows, pl.ds(0, bn)] = dpre
        n_out.start()

    @pl.when(jnp.logical_and(step > 0, step < nt))
    def _():
        act, dpre = gelu_pair(mm(n_v[...], up_ref[...]), mm(dy_v[...], down_ref[...], NT))
        act_ref[...] = act
        dpre_v[:, pl.ds(pl.multiple_of(step * bn, bn), bn)] = dpre

    @pl.when(step == nt - 2)
    def _():
        split.load(0).start()
        split.load(1).start()

    @pl.when(step == nt)
    def _():
        d_out.start()

    @pl.when(step >= nt)
    def _():
        split.tile(step - nt)

    @pl.when(step == nt + split.tiles)
    def _():
        n_out.wait()
        d_out.wait()


def mlp(m, h1, dy, stats, gain, w_up, w_down, token):
    _, seq, hid = h1.shape
    ffn = w_up.shape[1]
    bn, wide, chunks = 256, 1024, 4
    nt, tiles = ffn // bn, hid // wide
    col = lambda j: jnp.minimum(j, nt - 1)
    sum_specs, sums = Split.out(seq, hid, wide, nt)
    return call(
        partial(mlp_kernel, m, nt), (nt + tiles + 1,),
        [ANY, ANY, pl.BlockSpec((1, seq, 2), lambda j: (m, 0, 0)), pl.BlockSpec((1, hid), lambda j: (0, 0)),
         pl.BlockSpec((hid, bn), lambda j: (0, col(j))), pl.BlockSpec((bn, hid), lambda j: (col(j), 0)), ANY],
        [h1, dy, stats, gain, w_up, w_down, w_up],
        [ANY, pl.BlockSpec((seq, bn), lambda j: (0, col(j))), ANY] + sum_specs,
        [sds((seq, hid)), sds((seq, ffn)), sds((seq, ffn))] + sums, token, 6 * seq * hid * ffn,
        scratch=[pltpu.VMEM((seq, hid), BF16), pltpu.VMEM((seq, hid), BF16), pltpu.VMEM((seq, ffn), BF16),
                 pltpu.SemaphoreType.DMA((chunks,)), pltpu.SemaphoreType.DMA((chunks,)), pltpu.SemaphoreType.DMA((2,)),
                 *Split.scratch(seq, ffn, hid, wide)],
        name='mlp', cid=m)


def qkv_kernel(m, x_ref, st_ref, g_ref, w_ref, n_hbm, out_ref, n_v, x_sem, out_sem):
    step = pl.program_id(0)
    chunks = x_sem.shape[0]
    part = n_v.shape[0] // chunks
    n_out = pltpu.make_async_copy(n_v, n_hbm, out_sem)

    def load(r):
        rows = pl.ds(pl.multiple_of(r * part, part), part)
        return pltpu.make_async_copy(x_ref.at[m, rows], n_v.at[rows], x_sem.at[r])

    @pl.when(step == 0)
    def _():
        for r in range(chunks):
            load(r).start()

        @pl.loop(0, chunks)
        def _(r):
            rows = pl.ds(pl.multiple_of(r * part, part), part)
            load(r).wait()
            n_v[rows, :] = normed(n_v[rows, :], st_ref[0, rows, :], g_ref[...])
            out_ref[rows, :] = mm(n_v[rows, :], w_ref[...]).astype(BF16)
        n_out.start()

    @pl.when(step > 0)
    def _():
        out_ref[...] = mm(n_v[...], w_ref[...]).astype(BF16)

    @pl.when(step == pl.num_programs(0) - 1)
    def _():
        n_out.wait()


def qkv_proj(m, x, stats, gain, w, token):
    _, seq, hid = x.shape
    bn, chunks = 256, 4
    return call(
        partial(qkv_kernel, m), (w.shape[1] // bn,),
        [ANY, pl.BlockSpec((1, seq, 2), lambda j: (m, 0, 0)), pl.BlockSpec((1, hid), lambda j: (0, 0)),
         pl.BlockSpec((hid, bn), lambda j: (0, j))],
        [x, stats, gain, w], [ANY, pl.BlockSpec((seq, bn), lambda j: (0, j))],
        [sds((seq, hid)), sds((seq, w.shape[1]))], token, 2 * seq * hid * w.shape[1],
        scratch=[pltpu.VMEM((seq, hid), BF16), pltpu.SemaphoreType.DMA((chunks,)), pltpu.SemaphoreType.DMA],
        name='qkv')


def norm_kernel(pos_ref, keep_ref, r1_ref, r2_ref, r3_ref, act_ref, res_ref, st_ref, g_ref, out_ref):
    step = 16
    gain = g_ref[...].astype(F32)
    for i in range(keep_ref.shape[0] // step):
        rows = pl.ds(i * step, step)
        total = (keep_ref[rows, :] + r1_ref[rows, :].astype(F32) + r2_ref[rows, :].astype(F32)
                 + r3_ref[rows, :].astype(F32))
        rstd = st_ref[0, rows, 1:2]
        hat = (act_ref[0, rows, :].astype(F32) - st_ref[0, rows, 0:1]) * rstd
        scaled = total * gain
        mean_scaled = jnp.mean(scaled, axis=-1, keepdims=True)
        mean_cross = jnp.mean(scaled * hat, axis=-1, keepdims=True)
        res = (res_ref[0, rows, :] if len(res_ref.shape) == 3 else res_ref[rows, :]).astype(F32)
        out_ref[rows, :] = (res + rstd * (scaled - mean_scaled - hat * mean_cross)).astype(BF16)


def norm_shard(m, keep, got, acts, resid, stats, gain, pos, token):
    blk, hid = keep.shape
    bm = blk
    n = blk // bm
    local = pl.BlockSpec((bm, hid), lambda i, p: (i, 0))
    row = pl.BlockSpec((1, bm, hid), lambda i, p: (m, p[0] * n + i, 0))
    return call(
        norm_kernel, (n,),
        [local] * 4 + [row, row if resid.ndim == 3 else local,
                       pl.BlockSpec((1, bm, 2), lambda i, p: (m, p[0] * n + i, 0)), pl.BlockSpec((1, hid), lambda i, p: (0, 0))],
        [keep, *got, acts, resid, stats, gain], [local], [sds((blk, hid))], token, 20 * blk * hid, pos=pos, name='norm')


def head_backward(scale, q_ref, k_ref, v_ref, do_ref, o_ref, dq_ref, dk_ref, dv_ref, dk_acc, dv_acc):
    seq = do_ref.shape[0]
    k_all, v_all = k_ref[...], v_ref[...]
    k_t, v_t = k_all.T, v_all.T
    nblk = seq // BQ
    for i in reversed(range(nblk)):
        rows = pl.ds(i * BQ, BQ)
        width = (i + 1) * BQ
        q, do = q_ref[rows, :], do_ref[rows, :]
        s_t = mm(k_all[:width], q, NT) * scale
        kpos = lax.broadcasted_iota(jnp.int32, (width, BQ), 0)
        qpos = lax.broadcasted_iota(jnp.int32, (width, BQ), 1) + i * BQ
        s_t = jnp.where(qpos >= kpos, s_t, -1e30)
        top = jnp.max(s_t, axis=0, keepdims=True)
        p_t = jnp.exp(s_t - top)
        p_t = p_t * (1.0 / jnp.sum(p_t, axis=0, keepdims=True))
        p_b = p_t.astype(BF16)
        o_ref[rows, :] = mm(v_t[:, :width], p_b).T.astype(BF16)
        dp_t = mm(v_all[:width], do, NT)
        dot = jnp.sum(p_t * dp_t, axis=0, keepdims=True)
        ds_t = (p_t * (dp_t - dot) * scale).astype(BF16)
        dq_ref[rows, :] = mm(k_t[:, :width], ds_t).T.astype(BF16)
        dv, dk = mm(p_b, do), mm(ds_t, q)
        if i == nblk - 1:
            dv_acc[...] = dv
            dk_acc[...] = dk
        else:
            dv_acc[:width] += dv
            dk_acc[:width] += dk
    dk_ref[...] = dk_acc[...].astype(BF16)
    dv_ref[...] = dv_acc[...].astype(BF16)


def attn_kernel(scale, n, dh_ref, wo_ref, q_ref, k_ref, v_ref, w_hbm,
                o_ref, dq_ref, dk_ref, dv_ref, keep_ref, s1_ref, s2_ref, s3_ref,
                dh_v, do_v, g_v, dk_acc, dv_acc, dh_sem, *split_refs):
    step = pl.program_id(0)
    seq, dim = q_ref.shape
    chunks = dh_sem.shape[0]
    part = seq // chunks
    split = Split(g_v, w_hbm, (keep_ref, s1_ref, s2_ref, s3_ref), *split_refs)

    def load(r):
        rows = pl.ds(pl.multiple_of(r * part, part), part)
        return pltpu.make_async_copy(dh_ref.at[rows], dh_v.at[rows], dh_sem.at[r])

    @pl.when(step == 0)
    def _():
        for r in range(chunks):
            load(r).start()
        split.greet()

        @pl.loop(0, chunks)
        def _(r):
            rows = pl.ds(pl.multiple_of(r * part, part), part)
            load(r).wait()
            grad_o = mm(dh_v[rows, :], wo_ref[...], NT).astype(BF16)
            for h in range(n):
                do_v[h, rows, :] = grad_o[:, h * dim:(h + 1) * dim]
        split.load(0).start()
        split.load(1).start()

    @pl.when(step < n)
    def _():
        head_backward(scale, q_ref, k_ref, v_ref, do_v.at[step], o_ref, dq_ref, dk_ref, dv_ref, dk_acc, dv_acc)
        for c, ref in enumerate((dq_ref, dk_ref, dv_ref)):
            g_v[:, pl.ds(pl.multiple_of((c * n + step) * dim, dim), dim)] = ref[...]

    @pl.when(step >= n)
    def _():
        split.tile(step - n)


def attention(m, dh, w_out, qkv, w_flat, dim, scale, token):
    seq, hid = dh.shape
    width = w_out.shape[0]
    n = width // dim
    wide, chunks = 1024, 4
    head = lambda c: pl.BlockSpec((seq, dim), lambda i: (0, c * n + jnp.minimum(i, n - 1)))
    sum_specs, sums = Split.out(seq, hid, wide, n)
    return call(
        partial(attn_kernel, scale, n), (n + hid // wide + 1,),
        [ANY, pl.BlockSpec((width, hid), lambda i: (0, 0)), head(0), head(1), head(2), ANY],
        [dh, w_out, qkv, qkv, qkv, w_flat],
        [head(0)] * 4 + sum_specs, [sds((seq, width))] * 4 + sums, token,
        24 * n * seq * seq * dim + 8 * seq * hid * width,
        scratch=[pltpu.VMEM((seq, hid), BF16), pltpu.VMEM((n, seq, dim), BF16), pltpu.VMEM((seq, 3 * width), BF16),
                 pltpu.VMEM((seq, dim), F32), pltpu.VMEM((seq, dim), F32), pltpu.SemaphoreType.DMA((chunks,)),
                 *Split.scratch(seq, 3 * width, hid, wide)],
        name='attn', cid=2 + m)


def copy_kernel(src_ref, *refs):
    refs[-1][0] = src_ref[...]


def write_out(m, src, buf, count, token):
    seq, hid = src.shape
    bm = 256
    args, specs, alias = [src], [pl.BlockSpec((bm, hid), lambda i: (i, 0))], None
    if buf is not None:
        args, specs, alias = [src, buf], specs + [ANY], {1: 0}
    return call(copy_kernel, (seq // bm,), specs, args, [pl.BlockSpec((1, bm, hid), lambda i: (m, i, 0))],
                [sds((count, seq, hid))], token, src.size, alias=alias, name='copy')


def grad_kernel(a0_ref, a1_ref, b0_ref, b1_ref, out_ref):
    left = lambda ref: ref[0] if len(ref.shape) == 3 else ref[...]
    acc = mm(left(a0_ref), left(b0_ref), TN) + mm(left(a1_ref), left(b1_ref), TN)
    out_ref[...] = acc.astype(BF16)


def weight_grad(lhs, rhs, token, ba, bb, name):
    def split(v, size, axis):
        if isinstance(v, (list, tuple)):
            spec = pl.BlockSpec((v[0].shape[0], size), lambda i, j: (0, (i, j)[axis]))
            return list(v), [spec] * 2, v[0].shape
        specs = [pl.BlockSpec((1, v.shape[1], size), lambda i, j, m=m: (m, 0, (i, j)[axis])) for m in range(2)]
        return [v, v], specs, v.shape[1:]

    la, ls, (seq, wa) = split(lhs, ba, 0)
    ra, rs, (_, wb) = split(rhs, bb, 1)
    return call(grad_kernel, (wa // ba, wb // bb), ls + rs, la + ra, [pl.BlockSpec((ba, bb), lambda i, j: (i, j))],
                [sds((wa, wb))], token, 4 * seq * wa * wb, name=name)


def qkv_grad_kernel(a0_ref, a1_ref, *refs):
    out_ref = refs[-1]
    rows, _, heads, dim = out_ref.shape
    for c in range(3):
        acc = mm(a0_ref[...], refs[c][...], TN) + mm(a1_ref[...], refs[3 + c][...], TN)
        out_ref[:, c] = acc.reshape(rows, heads, dim).astype(BF16)


def qkv_grad(norms, grads, heads, dim, token):
    seq, hid = norms[0].shape
    ba = 1024
    lhs = pl.BlockSpec((seq, ba), lambda i: (0, i))
    whole = pl.BlockSpec((seq, heads * dim), lambda i: (0, 0))
    return call(qkv_grad_kernel, (hid // ba,), [lhs] * 2 + [whole] * 6, [*norms, *grads[0], *grads[1]],
                [pl.BlockSpec((ba, 3, heads, dim), lambda i: (i, 0, 0, 0))], [sds((hid, 3, heads, dim))], token,
                12 * seq * hid * heads * dim, name='dqkvw')


def flat_kernel(w_ref, out_ref):
    rows, _, heads, dim = w_ref.shape
    for c in range(3):
        out_ref[:, pl.ds(c * heads * dim, heads * dim)] = w_ref[:, c].reshape(rows, heads * dim)


def flat_weight(w, token):
    hid, three, heads, dim = w.shape
    bm = 256
    return call(flat_kernel, (hid // bm,), [pl.BlockSpec((bm, three, heads, dim), lambda i: (i, 0, 0, 0))], [w],
                [pl.BlockSpec((bm, three * heads * dim), lambda i: (i, 0))], [sds((hid, three * heads * dim))], token,
                w.size, name='flat')


def swap(arr, bit):
    return lax.ppermute(arr, 'tp', [(i, i ^ bit) for i in range(8)])


def solution(mesh):
    act_spec = P('dp', None, None)
    stat_spec = P('dp', None)
    in_specs = (act_spec, act_spec, act_spec, stat_spec, stat_spec, stat_spec, stat_spec, P(), P(),
                P(None, 'tp', None, None), P('tp', None, None), P(None, 'tp'), P('tp', None))
    out_specs = (act_spec, P('dp', 'tp', None, None), P(('dp', 'tp'), None, None), P('dp', 'tp'),
                 P(('dp', 'tp'), None))

    def local_backward(x_saved, h1_saved, grad_y, mean_one, rstd_one, mean_two, rstd_two,
                       gain_one, gain_two, w_qkv, w_out, w_up, w_down):
        hid, heads, _, dim = w_qkv.shape
        scale = dim ** -0.5
        idx = lax.axis_index('tp')
        pos = jnp.stack([idx, idx // 2, idx % 2]).astype(jnp.int32)
        stats_one = jnp.stack([mean_one, rstd_one], axis=-1)
        stats_two = jnp.stack([mean_two, rstd_two], axis=-1)
        g1, g2 = gain_one.reshape(1, hid), gain_two.reshape(1, hid)
        w_out = w_out.reshape(heads * dim, hid)
        tok = jnp.zeros((8, 128), F32)

        def gather(shard):
            return lax.all_gather(shard, 'tp', axis=0, tiled=True)

        def exchange(sends):
            return [swap(s, bit) for s, bit in zip(sends, (2, 4, 6))]

        n2, act, dpre, n1, qkv = [0, 0], [0, 0], [0, 0], [0, 0], [0, 0]
        dh_shard, dh, out, grads, dx = [0, 0], [0, 0], [0, 0], [0, 0], [0, 0]

        n2[0], act[0], dpre[0], keep_a, *send, tok = mlp(0, h1_saved, grad_y, stats_two, g2, w_up, w_down, tok)
        got_a = exchange(send)
        w_flat, tok = flat_weight(w_qkv.transpose(0, 2, 1, 3), tok)
        n1[0], qkv[0], tok = qkv_proj(0, x_saved, stats_one, g1, w_flat, tok)
        dh_shard[0], tok = norm_shard(0, keep_a, got_a, h1_saved, grad_y, stats_two, g2, pos, tok)
        dh[0] = gather(dh_shard[0])
        n2[1], act[1], dpre[1], keep_b, *send, tok = mlp(1, h1_saved, grad_y, stats_two, g2, w_up, w_down, tok)
        got_b = exchange(send)
        out[0], *g0, keep_a, s1, s2, s3, tok = attention(0, dh[0], w_out, qkv[0], w_flat, dim, scale, tok)
        got_a = exchange((s1, s2, s3))
        dh_shard[1], tok = norm_shard(1, keep_b, got_b, h1_saved, grad_y, stats_two, g2, pos, tok)
        dh[1] = gather(dh_shard[1])
        n1[1], qkv[1], tok = qkv_proj(1, x_saved, stats_one, g1, w_flat, tok)
        grad_down, tok = weight_grad(act, grad_y, tok, 1024, 1024, 'dw2')
        out[1], *g1s, keep_b, s1, s2, s3, tok = attention(1, dh[1], w_out, qkv[1], w_flat, dim, scale, tok)
        got_b = exchange((s1, s2, s3))
        dx_shard, tok = norm_shard(0, keep_a, got_a, x_saved, dh_shard[0], stats_one, g1, pos, tok)
        dx[0] = gather(dx_shard)
        grad_up, tok = weight_grad(n2, dpre, tok, 1024, 1024, 'dw1')
        dx_shard, tok = norm_shard(1, keep_b, got_b, x_saved, dh_shard[1], stats_one, g1, pos, tok)
        dx[1] = gather(dx_shard)
        grad_qkv_w, tok = qkv_grad(n1, [g0, g1s], heads, dim, tok)
        grad_out_w, tok = weight_grad(out, dh, tok, 512, 1024, 'dwo')
        grad_x, tok = write_out(0, dx[0], None, 2, tok)
        grad_x, tok = write_out(1, dx[1], grad_x, 2, tok)
        return grad_x, grad_qkv_w.transpose(0, 2, 1, 3), grad_out_w.reshape(heads, dim, hid), grad_up, grad_down

    return jax.shard_map(local_backward, mesh=mesh, in_specs=in_specs, out_specs=out_specs, check_vma=False)
```

```python
import jax
import jax.numpy as jnp
from jax import lax
from jax.sharding import PartitionSpec as P
from jax.experimental import pallas as pl
from jax.experimental.pallas import tpu as pltpu
from functools import partial

GELU_C = 0.7978845608028654
GELU_A = 0.044715
F32 = jnp.float32
BF16 = jnp.bfloat16
BQ = 256
NT = (((1,), (1,)), ((), ()))
TN = (((0,), (0,)), ((), ()))
ANY = pl.BlockSpec(memory_space=pl.ANY)
TOKEN = jax.ShapeDtypeStruct((8, 128), F32)


def mm(a, b, dims=(((1,), (0,)), ((), ()))):
    return lax.dot_general(a, b, dims, preferred_element_type=F32)


def call(body, grid, in_specs, args, out_specs, outs, token, flops, scratch=(), pos=None, name=None, alias=None, cid=None):
    n_in, n_out, n_pos = len(args), len(outs), 0 if pos is None else 1

    def kernel(*refs):
        head, refs = refs[:n_pos], refs[n_pos:]
        body(*head, *refs[:n_in], *refs[n_in + 1:n_in + 1 + n_out], *refs[n_in + 2 + n_out:])

    size = sum(o.size * o.dtype.itemsize for o in outs) + sum(a.size * a.dtype.itemsize for a in args)
    results = pl.pallas_call(
        kernel,
        grid_spec=pltpu.PrefetchScalarGridSpec(
            num_scalar_prefetch=n_pos, grid=grid, in_specs=list(in_specs) + [ANY],
            out_specs=list(out_specs) + [ANY], scratch_shapes=list(scratch)),
        out_shape=list(outs) + [TOKEN],
        compiler_params=pltpu.CompilerParams(vmem_limit_bytes=62 * 1024 * 1024, collective_id=cid, has_side_effects=cid is not None),
        cost_estimate=pl.CostEstimate(flops=int(flops), bytes_accessed=int(size), transcendentals=0),
        input_output_aliases=alias or {},
        name=name,
    )(*([] if pos is None else [pos]), *args, token)
    return results


def whole(arr):
    return pl.BlockSpec(arr.shape, lambda *ids: (0,) * arr.ndim)


def sds(shape, dtype=BF16):
    return jax.ShapeDtypeStruct(shape, dtype)


def column(row):
    return jnp.broadcast_to(row, (8, row.shape[1])).T[:, 0:1]


def normed(rows, mean, rstd, gain):
    return ((rows.astype(F32) - column(mean)) * column(rstd) * gain.astype(F32)).astype(BF16)


class Split:
    def __init__(self, lhs, w_hbm, outs, wrow, prod, got, w_sem, send_sem, recv_sem):
        self.lhs, self.w_hbm, self.outs = lhs, w_hbm, outs
        self.wrow, self.prod, self.got = wrow, prod, got
        self.w_sem, self.send_sem, self.recv_sem = w_sem, send_sem, recv_sem
        self.wide = wrow.shape[1]
        self.tiles = w_hbm.shape[0] // self.wide
        self.blk = prod.shape[1] // 8
        idx = lax.axis_index('tp')
        self.chip, self.core = lax.div(idx, 2), lax.rem(idx, 2)
        self.partner = 2 * self.chip + 1 - self.core

    def load(self, t):
        return pltpu.make_async_copy(self.w_hbm.at[pl.ds(t * self.wide, self.wide), :], self.wrow.at[t % 2],
                                     self.w_sem.at[t % 2])

    def rows(self, k, core):
        return pl.ds(pl.multiple_of((2 * lax.bitwise_xor(self.chip, k) + core) * self.blk, self.blk), self.blk)

    def send(self, t, k):
        return pltpu.make_async_remote_copy(
            src_ref=self.prod.at[t % 2, self.rows(k, 1 - self.core)], dst_ref=self.got.at[t, k],
            send_sem=self.send_sem.at[t, k], recv_sem=self.recv_sem.at[t, k],
            device_id={'tp': self.partner}, device_id_type=pl.DeviceIdType.MESH)

    def greet(self):
        barrier = pltpu.get_barrier_semaphore()
        pl.semaphore_signal(barrier, inc=1, device_id={'tp': self.partner}, device_id_type=pl.DeviceIdType.MESH)
        pl.semaphore_wait(barrier, 1)

    def tile(self, t):
        @pl.when(t < self.tiles)
        def _():
            self.load(t).wait()

            @pl.when(t >= 2)
            def _():
                for k in range(4):
                    self.send(t - 2, k).wait_send()

            self.prod[t % 2] = mm(self.lhs[...], self.wrow[t % 2], NT).astype(BF16)
            for k in range(4):
                self.send(t, k).start()

            @pl.when(t + 2 < self.tiles)
            def _():
                self.load(t + 2).start()

        @pl.when(t > 0)
        def _():
            for k in range(4):
                self.send(t - 1, k).wait_recv()
                total = self.prod[(t - 1) % 2, self.rows(k, self.core)].astype(F32) + self.got[t - 1, k].astype(F32)
                self.outs[k][...] = total.astype(self.outs[k].dtype)

        @pl.when(t == self.tiles)
        def _():
            for u in range(self.tiles - 2, self.tiles):
                for k in range(4):
                    self.send(u, k).wait_send()

    @staticmethod
    def scratch(seq, depth, hid, wide):
        tiles = hid // wide
        return [pltpu.VMEM((2, wide, depth), BF16), pltpu.VMEM((2, seq, wide), BF16),
                pltpu.VMEM((tiles, 4, seq // 8, wide), BF16), pltpu.SemaphoreType.DMA((2,)),
                pltpu.SemaphoreType.DMA((tiles, 4)), pltpu.SemaphoreType.DMA((tiles, 4))]

    @staticmethod
    def out(seq, hid, wide, first):
        last = hid // wide - 1
        spec = pl.BlockSpec((seq // 8, wide), lambda j: (0, jnp.clip(j - first - 1, 0, last)))
        return [spec] * 4, [sds((seq // 8, hid), F32)] + [sds((seq // 8, hid))] * 3


def gelu_pair(a, b):
    tanh = jnp.tanh(GELU_C * (a + GELU_A * a * a * a))
    slope = (0.5 * (1.0 + tanh)
             + 0.5 * a * (1.0 - tanh * tanh) * GELU_C * (1.0 + 3.0 * GELU_A * a * a))
    return (0.5 * a * (1.0 + tanh)).astype(BF16), (b * slope).astype(BF16)


def mlp_kernel(m, nt, h_ref, dy_ref, mu_ref, rs_ref, g_ref, up_ref, down_ref, up_hbm,
               n_hbm, act_ref, dpre_hbm, keep_ref, s1_ref, s2_ref, s3_ref,
               n_v, dy_v, dpre_v, a_v, b_v, h_sem, dy_sem, out_sem, *split_refs):
    step = pl.program_id(0)
    bn = up_ref.shape[1]
    chunks = h_sem.shape[0]
    part = n_v.shape[0] // chunks
    split = Split(dpre_v, up_hbm, (keep_ref, s1_ref, s2_ref, s3_ref), *split_refs)
    n_out = pltpu.make_async_copy(n_v, n_hbm, out_sem.at[0])
    d_out = pltpu.make_async_copy(dpre_v, dpre_hbm, out_sem.at[1])

    def load(r):
        rows = pl.ds(pl.multiple_of(r * part, part), part)
        return (pltpu.make_async_copy(h_ref.at[m, rows], n_v.at[rows], h_sem.at[r]),
                pltpu.make_async_copy(dy_ref.at[m, rows], dy_v.at[rows], dy_sem.at[r]))

    @pl.when(step == 0)
    def _():
        for r in range(chunks):
            for copy in load(r):
                copy.start()
        split.greet()

        @pl.loop(0, chunks)
        def _(r):
            rows = pl.ds(pl.multiple_of(r * part, part), part)
            h_copy, dy_copy = load(r)
            h_copy.wait()
            n_v[rows, :] = normed(n_v[rows, :], mu_ref[m:m + 1, rows], rs_ref[m:m + 1, rows], g_ref[...])
            dy_copy.wait()
            a_v[rows, :] = mm(n_v[rows, :], up_ref[...])
            b_v[rows, :] = mm(dy_v[rows, :], down_ref[...], NT)

        n_out.start()

    def finish():
        act, dpre = gelu_pair(a_v[...], b_v[...])
        act_ref[...] = act
        dpre_v[:, pl.ds(pl.multiple_of((step - 1) * bn, bn), bn)] = dpre

    @pl.when(jnp.logical_and(step > 0, step < nt))
    def _():
        finish()
        a_v[...] = mm(n_v[...], up_ref[...])
        b_v[...] = mm(dy_v[...], down_ref[...], NT)

    @pl.when(step == nt - 2)
    def _():
        split.load(0).start()
        split.load(1).start()

    @pl.when(step == nt)
    def _():
        finish()
        d_out.start()

    @pl.when(step >= nt)
    def _():
        split.tile(step - nt)

    @pl.when(step == nt + split.tiles)
    def _():
        n_out.wait()
        d_out.wait()


def mlp(m, h1, dy, stats, gain, w_up, w_down, token):
    _, seq, hid = h1.shape
    ffn = w_up.shape[1]
    bn, wide, chunks = 256, 1024, 4
    nt, tiles = ffn // bn, hid // wide
    col = lambda j: jnp.minimum(j, nt - 1)
    sum_specs, sums = Split.out(seq, hid, wide, nt)
    return call(
        partial(mlp_kernel, m, nt), (nt + tiles + 1,),
        [ANY, ANY, whole(stats[0]), whole(stats[1]), whole(gain),
         pl.BlockSpec((hid, bn), lambda j: (0, col(j))), pl.BlockSpec((bn, hid), lambda j: (col(j), 0)), ANY],
        [h1, dy, *stats, gain, w_up, w_down, w_up],
        [ANY, pl.BlockSpec((seq, bn), lambda j: (0, jnp.clip(j - 1, 0, nt - 1))), ANY] + sum_specs,
        [sds((seq, hid)), sds((seq, ffn)), sds((seq, ffn))] + sums, token, 6 * seq * hid * ffn,
        scratch=[pltpu.VMEM((seq, hid), BF16), pltpu.VMEM((seq, hid), BF16), pltpu.VMEM((seq, ffn), BF16),
                 pltpu.VMEM((seq, bn), F32), pltpu.VMEM((seq, bn), F32),
                 pltpu.SemaphoreType.DMA((chunks,)), pltpu.SemaphoreType.DMA((chunks,)), pltpu.SemaphoreType.DMA((2,)),
                 *Split.scratch(seq, ffn, hid, wide)],
        name='mlp', cid=m)


def qkv_kernel(m, x_ref, mu_ref, rs_ref, g_ref, w_ref, n_hbm, out_ref, n_v, x_sem, out_sem):
    step = pl.program_id(0)
    chunks = x_sem.shape[0]
    part = n_v.shape[0] // chunks
    n_out = pltpu.make_async_copy(n_v, n_hbm, out_sem)

    def load(r):
        rows = pl.ds(pl.multiple_of(r * part, part), part)
        return pltpu.make_async_copy(x_ref.at[m, rows], n_v.at[rows], x_sem.at[r])

    @pl.when(step == 0)
    def _():
        for r in range(chunks):
            load(r).start()

        @pl.loop(0, chunks)
        def _(r):
            rows = pl.ds(pl.multiple_of(r * part, part), part)
            load(r).wait()
            n_v[rows, :] = normed(n_v[rows, :], mu_ref[m:m + 1, rows], rs_ref[m:m + 1, rows], g_ref[...])
            out_ref[rows, :] = mm(n_v[rows, :], w_ref[...]).astype(BF16)
        n_out.start()

    @pl.when(step > 0)
    def _():
        out_ref[...] = mm(n_v[...], w_ref[...]).astype(BF16)

    @pl.when(step == pl.num_programs(0) - 1)
    def _():
        n_out.wait()


def qkv_proj(m, x, stats, gain, w, token):
    _, seq, hid = x.shape
    bn, chunks = 256, 4
    return call(
        partial(qkv_kernel, m), (w.shape[1] // bn,),
        [ANY, whole(stats[0]), whole(stats[1]), whole(gain),
         pl.BlockSpec((hid, bn), lambda j: (0, j))],
        [x, *stats, gain, w], [ANY, pl.BlockSpec((seq, bn), lambda j: (0, j))],
        [sds((seq, hid)), sds((seq, w.shape[1]))], token, 2 * seq * hid * w.shape[1],
        scratch=[pltpu.VMEM((seq, hid), BF16), pltpu.SemaphoreType.DMA((chunks,)), pltpu.SemaphoreType.DMA],
        name='qkv')


def norm_kernel(m, pos_ref, keep_ref, r1_ref, r2_ref, r3_ref, act_ref, res_ref, mu_ref, rs_ref, g_ref, out_ref,
                mu_v, rs_v):
    blk, hid = keep_ref.shape
    high, wide = 16, 512
    mu_v[...] = jnp.broadcast_to(mu_ref[m:m + 1, :], (128, blk)).T
    rs_v[...] = jnp.broadcast_to(rs_ref[m:m + 1, :], (128, blk)).T

    @pl.loop(0, blk // high)
    def _(i):
        rows = pl.ds(pl.multiple_of(i * high, high), high)
        mean, rstd = mu_v[rows, 0:1], rs_v[rows, 0:1]

        def terms(j):
            cols = pl.ds(j * wide, wide)
            total = (keep_ref[rows, cols] + r1_ref[rows, cols].astype(F32) + r2_ref[rows, cols].astype(F32)
                     + r3_ref[rows, cols].astype(F32))
            hat = (act_ref[0, rows, cols].astype(F32) - mean) * rstd
            return cols, total * g_ref[:, cols].astype(F32), hat

        plain = cross = jnp.zeros((high, wide), F32)
        for j in range(hid // wide):
            _, scaled, hat = terms(j)
            plain = plain + scaled
            cross = cross + scaled * hat
        mean_scaled = jnp.sum(plain, axis=-1, keepdims=True) * (1.0 / hid)
        mean_cross = jnp.sum(cross, axis=-1, keepdims=True) * (1.0 / hid)
        for j in range(hid // wide):
            cols, scaled, hat = terms(j)
            res = (res_ref[0, rows, cols] if len(res_ref.shape) == 3 else res_ref[rows, cols]).astype(F32)
            out_ref[rows, cols] = (res + rstd * (scaled - mean_scaled - hat * mean_cross)).astype(BF16)


def norm_shard(m, keep, got, acts, resid, stats, gain, pos, token):
    blk, hid = keep.shape
    local = pl.BlockSpec((blk, hid), lambda i, p: (0, 0))
    row = pl.BlockSpec((1, blk, hid), lambda i, p: (m, p[0], 0))
    stat = pl.BlockSpec((stats[0].shape[0], blk), lambda i, p: (0, p[0]))
    return call(
        partial(norm_kernel, m), (1,),
        [local] * 4 + [row, row if resid.ndim == 3 else local, stat, stat, whole(gain)],
        [keep, *got, acts, resid, *stats, gain], [local], [sds((blk, hid))], token, 20 * blk * hid,
        scratch=[pltpu.VMEM((blk, 128), F32)] * 2, pos=pos, name='norm')


def head_backward(scale, q_ref, k_ref, v_ref, do_ref, o_ref, dq_ref, dk_ref, dv_ref, dk_acc, dv_acc):
    seq = do_ref.shape[0]
    k_all, v_all = k_ref[...], v_ref[...]
    k_t, v_t = k_all.T, v_all.T
    nblk = seq // BQ
    kpos = lax.broadcasted_iota(jnp.int32, (BQ, BQ), 0)
    qpos = lax.broadcasted_iota(jnp.int32, (BQ, BQ), 1)
    for i in reversed(range(nblk)):
        rows = pl.ds(i * BQ, BQ)
        width = (i + 1) * BQ
        q, do = q_ref[rows, :], do_ref[rows, :]
        s_t = mm(k_all[:width], q, NT)
        last = jnp.where(qpos >= kpos, s_t[i * BQ:], -1e30)
        s_t = jnp.concatenate([s_t[:i * BQ], last], axis=0) if i else last
        top = jnp.max(s_t, axis=0, keepdims=True)
        p_t = jnp.exp((s_t - top) * scale)
        p_t = p_t * (1.0 / jnp.sum(p_t, axis=0, keepdims=True))
        p_b = p_t.astype(BF16)
        o_ref[rows, :] = mm(v_t[:, :width], p_b).T.astype(BF16)
        dp_t = mm(v_all[:width], do, NT)
        dot = jnp.sum(p_t * dp_t, axis=0, keepdims=True)
        ds_t = (p_t * (dp_t - dot) * scale).astype(BF16)
        dq_ref[rows, :] = mm(k_t[:, :width], ds_t).T.astype(BF16)
        dv, dk = mm(p_b, do), mm(ds_t, q)
        if i == nblk - 1:
            dv_acc[...] = dv
            dk_acc[...] = dk
        else:
            dv_acc[:width] += dv
            dk_acc[:width] += dk
    dk_ref[...] = dk_acc[...].astype(BF16)
    dv_ref[...] = dv_acc[...].astype(BF16)


def attn_kernel(scale, n, dh_ref, wo_ref, q_ref, k_ref, v_ref, w_hbm,
                o_ref, dq_ref, dk_ref, dv_ref, keep_ref, s1_ref, s2_ref, s3_ref,
                dh_v, do_v, g_v, dk_acc, dv_acc, dh_sem, *split_refs):
    step = pl.program_id(0)
    seq, dim = q_ref.shape
    chunks = dh_sem.shape[0]
    part = seq // chunks
    split = Split(g_v, w_hbm, (keep_ref, s1_ref, s2_ref, s3_ref), *split_refs)

    def load(r):
        rows = pl.ds(pl.multiple_of(r * part, part), part)
        return pltpu.make_async_copy(dh_ref.at[rows], dh_v.at[rows], dh_sem.at[r])

    @pl.when(step == 0)
    def _():
        for r in range(chunks):
            load(r).start()
        split.greet()

        @pl.loop(0, chunks)
        def _(r):
            rows = pl.ds(pl.multiple_of(r * part, part), part)
            load(r).wait()
            grad_o = mm(dh_v[rows, :], wo_ref[...], NT).astype(BF16)
            for h in range(n):
                do_v[h, rows, :] = grad_o[:, h * dim:(h + 1) * dim]
        split.load(0).start()
        split.load(1).start()

    @pl.when(step < n)
    def _():
        head_backward(scale, q_ref, k_ref, v_ref, do_v.at[step], o_ref, dq_ref, dk_ref, dv_ref, dk_acc, dv_acc)
        for c, ref in enumerate((dq_ref, dk_ref, dv_ref)):
            g_v[:, pl.ds(pl.multiple_of((c * n + step) * dim, dim), dim)] = ref[...]

    @pl.when(step >= n)
    def _():
        split.tile(step - n)


def attention(m, dh, w_out, qkv, w_flat, dim, scale, token):
    seq, hid = dh.shape
    width = w_out.shape[0]
    n = width // dim
    wide, chunks = 1024, 4
    head = lambda c: pl.BlockSpec((seq, dim), lambda i: (0, c * n + jnp.minimum(i, n - 1)))
    sum_specs, sums = Split.out(seq, hid, wide, n)
    return call(
        partial(attn_kernel, scale, n), (n + hid // wide + 1,),
        [ANY, pl.BlockSpec((width, hid), lambda i: (0, 0)), head(0), head(1), head(2), ANY],
        [dh, w_out, qkv, qkv, qkv, w_flat],
        [head(0)] * 4 + sum_specs, [sds((seq, width))] * 4 + sums, token,
        24 * n * seq * seq * dim + 8 * seq * hid * width,
        scratch=[pltpu.VMEM((seq, hid), BF16), pltpu.VMEM((n, seq, dim), BF16), pltpu.VMEM((seq, 3 * width), BF16),
                 pltpu.VMEM((seq, dim), F32), pltpu.VMEM((seq, dim), F32), pltpu.SemaphoreType.DMA((chunks,)),
                 *Split.scratch(seq, 3 * width, hid, wide)],
        name='attn', cid=2 + m)


def copy_kernel(m, src, old, dst, buf, in_sem, out_sem):
    parts = in_sem.shape[0]
    part = src.shape[0] // parts
    at = [pl.ds(r * part, part) for r in range(parts)]
    loads = [pltpu.make_async_copy(src.at[at[r]], buf.at[at[r]], in_sem.at[r]) for r in range(parts)]
    stores = [pltpu.make_async_copy(buf.at[at[r]], dst.at[m, at[r]], out_sem.at[r]) for r in range(parts)]
    for load in loads:
        load.start()
    for load, store in zip(loads, stores):
        load.wait()
        store.start()
    for store in stores:
        store.wait()


def write_out(m, src, old, token):
    parts = 8
    return call(partial(copy_kernel, m), (1,), [ANY, ANY], [src, old], [ANY], [sds(old.shape)], token, src.size,
                scratch=[pltpu.VMEM(src.shape, BF16), pltpu.SemaphoreType.DMA((parts,)),
                         pltpu.SemaphoreType.DMA((parts,))], alias={1: 0}, name='copy')


def grad_kernel(a0_ref, a1_ref, b0_ref, b1_ref, out_ref):
    left = lambda ref: ref[0] if len(ref.shape) == 3 else ref[...]
    acc = mm(left(a0_ref), left(b0_ref), TN) + mm(left(a1_ref), left(b1_ref), TN)
    out_ref[...] = acc.astype(BF16)


def weight_grad(lhs, rhs, token, ba, bb, name):
    def split(v, size, axis):
        if isinstance(v, (list, tuple)):
            spec = pl.BlockSpec((v[0].shape[0], size), lambda i, j: (0, (i, j)[axis]))
            return list(v), [spec] * 2, v[0].shape
        specs = [pl.BlockSpec((1, v.shape[1], size), lambda i, j, m=m: (m, 0, (i, j)[axis])) for m in range(2)]
        return [v, v], specs, v.shape[1:]

    la, ls, (seq, wa) = split(lhs, ba, 0)
    ra, rs, (_, wb) = split(rhs, bb, 1)
    return call(grad_kernel, (wa // ba, wb // bb), ls + rs, la + ra, [pl.BlockSpec((ba, bb), lambda i, j: (i, j))],
                [sds((wa, wb))], token, 4 * seq * wa * wb, name=name)


def qkv_grad_kernel(a0_ref, a1_ref, *refs):
    src, out_ref, dst, buf, in_sem, out_sem = refs[6], *refs[7:]
    rows, _, heads, dim = out_ref.shape
    step, steps = pl.program_id(0), pl.num_programs(0)
    part = src.shape[0] // in_sem.shape[0]

    def move(r, out):
        at = pl.ds(r * part, part)
        if out:
            return pltpu.make_async_copy(buf.at[at], dst.at[0, at], out_sem.at[r])
        return pltpu.make_async_copy(src.at[at], buf.at[at], in_sem.at[r])

    for r in range(in_sem.shape[0]):
        @pl.when(step == r)
        def _():
            move(r, False).start()

        @pl.when(step == r + 1)
        def _():
            move(r, False).wait()
            move(r, True).start()

    for c in range(3):
        acc = mm(a0_ref[...], refs[c][...], TN) + mm(a1_ref[...], refs[3 + c][...], TN)
        out_ref[:, c] = acc.reshape(rows, heads, dim).astype(BF16)

    @pl.when(step == steps - 1)
    def _():
        for r in range(in_sem.shape[0]):
            move(r, True).wait()


def qkv_grad(norms, grads, heads, dim, dx, count, token):
    seq, hid = norms[0].shape
    ba, parts = 512, 4
    lhs = pl.BlockSpec((seq, ba), lambda i: (0, i))
    rhs = pl.BlockSpec((seq, heads * dim), lambda i: (0, 0))
    return call(qkv_grad_kernel, (hid // ba,), [lhs] * 2 + [rhs] * 6 + [ANY], [*norms, *grads[0], *grads[1], dx],
                [pl.BlockSpec((ba, 3, heads, dim), lambda i: (i, 0, 0, 0)), ANY],
                [sds((hid, 3, heads, dim)), sds((count, *dx.shape))], token, 12 * seq * hid * heads * dim,
                scratch=[pltpu.VMEM(dx.shape, BF16), pltpu.SemaphoreType.DMA((parts,)),
                         pltpu.SemaphoreType.DMA((parts,))], name='dqkvw')


def flat_kernel(w_ref, out_ref):
    rows, _, heads, dim = w_ref.shape
    for c in range(3):
        out_ref[:, pl.ds(c * heads * dim, heads * dim)] = w_ref[:, c].reshape(rows, heads * dim)


def flat_weight(w, token):
    hid, three, heads, dim = w.shape
    bm = 256
    return call(flat_kernel, (hid // bm,), [pl.BlockSpec((bm, three, heads, dim), lambda i: (i, 0, 0, 0))], [w],
                [pl.BlockSpec((bm, three * heads * dim), lambda i: (i, 0))], [sds((hid, three * heads * dim))], token,
                w.size, name='flat')


def swap(arr, bit):
    return lax.ppermute(arr, 'tp', [(i, i ^ bit) for i in range(8)])


def solution(mesh):
    act_spec = P('dp', None, None)
    stat_spec = P('dp', None)
    in_specs = (act_spec, act_spec, act_spec, stat_spec, stat_spec, stat_spec, stat_spec, P(), P(),
                P(None, 'tp', None, None), P('tp', None, None), P(None, 'tp'), P('tp', None))
    out_specs = (act_spec, P('dp', 'tp', None, None), P(('dp', 'tp'), None, None), P('dp', 'tp'),
                 P(('dp', 'tp'), None))

    def local_backward(x_saved, h1_saved, grad_y, mean_one, rstd_one, mean_two, rstd_two,
                       gain_one, gain_two, w_qkv, w_out, w_up, w_down):
        hid, heads, _, dim = w_qkv.shape
        scale = dim ** -0.5
        idx = lax.axis_index('tp')
        pos = jnp.stack([idx, idx // 2, idx % 2]).astype(jnp.int32)
        stats_one, stats_two = (mean_one, rstd_one), (mean_two, rstd_two)
        g1, g2 = gain_one.reshape(1, hid), gain_two.reshape(1, hid)
        w_out = w_out.reshape(heads * dim, hid)
        tok = jnp.zeros((8, 128), F32)

        def gather(shard):
            return lax.all_gather(shard, 'tp', axis=0, tiled=True)

        def exchange(sends):
            return [swap(s, bit) for s, bit in zip(sends, (2, 4, 6))]

        n2, act, dpre, n1, qkv = [0, 0], [0, 0], [0, 0], [0, 0], [0, 0]
        dh_shard, dh, out, grads, dx = [0, 0], [0, 0], [0, 0], [0, 0], [0, 0]

        n2[0], act[0], dpre[0], keep_a, *send, tok = mlp(0, h1_saved, grad_y, stats_two, g2, w_up, w_down, tok)
        got_a = exchange(send)
        w_flat, tok = flat_weight(w_qkv.transpose(0, 2, 1, 3), tok)
        n1[0], qkv[0], tok = qkv_proj(0, x_saved, stats_one, g1, w_flat, tok)
        dh_shard[0], tok = norm_shard(0, keep_a, got_a, h1_saved, grad_y, stats_two, g2, pos, tok)
        dh[0] = gather(dh_shard[0])
        n2[1], act[1], dpre[1], keep_b, *send, tok = mlp(1, h1_saved, grad_y, stats_two, g2, w_up, w_down, tok)
        got_b = exchange(send)
        out[0], *g0, keep_a, s1, s2, s3, tok = attention(0, dh[0], w_out, qkv[0], w_flat, dim, scale, tok)
        got_a = exchange((s1, s2, s3))
        dh_shard[1], tok = norm_shard(1, keep_b, got_b, h1_saved, grad_y, stats_two, g2, pos, tok)
        dh[1] = gather(dh_shard[1])
        n1[1], qkv[1], tok = qkv_proj(1, x_saved, stats_one, g1, w_flat, tok)
        grad_down, tok = weight_grad(act, grad_y, tok, 1024, 1024, 'dw2')
        dx_shard, tok = norm_shard(0, keep_a, got_a, x_saved, dh_shard[0], stats_one, g1, pos, tok)
        dx[0] = gather(dx_shard)
        out[1], *g1s, keep_b, s1, s2, s3, tok = attention(1, dh[1], w_out, qkv[1], w_flat, dim, scale, tok)
        got_b = exchange((s1, s2, s3))
        grad_up, tok = weight_grad(n2, dpre, tok, 1024, 1024, 'dw1')
        dx_shard, tok = norm_shard(1, keep_b, got_b, x_saved, dh_shard[1], stats_one, g1, pos, tok)
        dx[1] = gather(dx_shard)
        grad_out_w, tok = weight_grad(out, dh, tok, 512, 1024, 'dwo')
        grad_qkv_w, grad_x, tok = qkv_grad(n1, [g0, g1s], heads, dim, dx[0], 2, tok)
        grad_x, tok = write_out(1, dx[1], grad_x, tok)
        return grad_x, grad_qkv_w.transpose(0, 2, 1, 3), grad_out_w.reshape(heads, dim, hid), grad_up, grad_down

    return jax.shard_map(local_backward, mesh=mesh, in_specs=in_specs, out_specs=out_specs, check_vma=False)
```

```python
import jax
import jax.numpy as jnp
from jax import lax
from jax.sharding import PartitionSpec as P
from jax.experimental import pallas as pl
from jax.experimental.pallas import tpu as pltpu
from functools import partial

GELU_C = 0.7978845608028654
GELU_A = 0.044715
F32 = jnp.float32
BF16 = jnp.bfloat16
BQ = 256
NT = (((1,), (1,)), ((), ()))
TN = (((0,), (0,)), ((), ()))
ANY = pl.BlockSpec(memory_space=pl.ANY)
TOKEN = jax.ShapeDtypeStruct((8, 128), F32)


def mm(a, b, dims=(((1,), (0,)), ((), ()))):
    return lax.dot_general(a, b, dims, preferred_element_type=F32)


def call(body, grid, in_specs, args, out_specs, outs, token, flops, scratch=(), pos=None, name=None, alias=None, cid=None):
    n_in, n_out, n_pos = len(args), len(outs), 0 if pos is None else 1

    def kernel(*refs):
        head, refs = refs[:n_pos], refs[n_pos:]
        body(*head, *refs[:n_in], *refs[n_in + 1:n_in + 1 + n_out], *refs[n_in + 2 + n_out:])

    size = sum(o.size * o.dtype.itemsize for o in outs) + sum(a.size * a.dtype.itemsize for a in args)
    results = pl.pallas_call(
        kernel,
        grid_spec=pltpu.PrefetchScalarGridSpec(
            num_scalar_prefetch=n_pos, grid=grid, in_specs=list(in_specs) + [ANY],
            out_specs=list(out_specs) + [ANY], scratch_shapes=list(scratch)),
        out_shape=list(outs) + [TOKEN],
        compiler_params=pltpu.CompilerParams(vmem_limit_bytes=62 * 1024 * 1024, collective_id=cid, has_side_effects=cid is not None),
        cost_estimate=pl.CostEstimate(flops=int(flops), bytes_accessed=int(size), transcendentals=0),
        input_output_aliases=alias or {},
        name=name,
    )(*([] if pos is None else [pos]), *args, token)
    return results


def whole(arr):
    return pl.BlockSpec(arr.shape, lambda *ids: (0,) * arr.ndim)


def sds(shape, dtype=BF16):
    return jax.ShapeDtypeStruct(shape, dtype)


def column(row):
    return jnp.broadcast_to(row, (8, row.shape[1])).T[:, 0:1]


def normed(rows, mean, rstd, gain):
    return ((rows.astype(F32) - column(mean)) * column(rstd) * gain.astype(F32)).astype(BF16)


class Split:
    def __init__(self, lhs, w_hbm, outs, wrow, prod, got, w_sem, send_sem, recv_sem):
        self.lhs, self.w_hbm, self.outs = lhs, w_hbm, outs
        self.wrow, self.prod, self.got = wrow, prod, got
        self.w_sem, self.send_sem, self.recv_sem = w_sem, send_sem, recv_sem
        self.wide = wrow.shape[1]
        self.tiles = w_hbm.shape[0] // self.wide
        self.blk = prod.shape[1] // 8
        idx = lax.axis_index('tp')
        self.chip, self.core = lax.div(idx, 2), lax.rem(idx, 2)
        self.partner = 2 * self.chip + 1 - self.core

    def load(self, t):
        return pltpu.make_async_copy(self.w_hbm.at[pl.ds(t * self.wide, self.wide), :], self.wrow.at[t % 2],
                                     self.w_sem.at[t % 2])

    def rows(self, k, core):
        return pl.ds(pl.multiple_of((2 * lax.bitwise_xor(self.chip, k) + core) * self.blk, self.blk), self.blk)

    def send(self, t, k):
        return pltpu.make_async_remote_copy(
            src_ref=self.prod.at[t % 2, self.rows(k, 1 - self.core)], dst_ref=self.got.at[t, k],
            send_sem=self.send_sem.at[t, k], recv_sem=self.recv_sem.at[t, k],
            device_id={'tp': self.partner}, device_id_type=pl.DeviceIdType.MESH)

    def greet(self):
        barrier = pltpu.get_barrier_semaphore()
        pl.semaphore_signal(barrier, inc=1, device_id={'tp': self.partner}, device_id_type=pl.DeviceIdType.MESH)
        pl.semaphore_wait(barrier, 1)

    def tile(self, t):
        @pl.when(t < self.tiles)
        def _():
            self.load(t).wait()

            @pl.when(t >= 2)
            def _():
                for k in range(4):
                    self.send(t - 2, k).wait_send()

            self.prod[t % 2] = mm(self.lhs[...], self.wrow[t % 2], NT).astype(BF16)
            for k in range(4):
                self.send(t, k).start()

            @pl.when(t + 2 < self.tiles)
            def _():
                self.load(t + 2).start()

        @pl.when(t > 0)
        def _():
            for k in range(4):
                self.send(t - 1, k).wait_recv()
                total = self.prod[(t - 1) % 2, self.rows(k, self.core)].astype(F32) + self.got[t - 1, k].astype(F32)
                self.outs[k][...] = total.astype(self.outs[k].dtype)

        @pl.when(t == self.tiles)
        def _():
            for u in range(self.tiles - 2, self.tiles):
                for k in range(4):
                    self.send(u, k).wait_send()

    @staticmethod
    def scratch(seq, depth, hid, wide):
        tiles = hid // wide
        return [pltpu.VMEM((2, wide, depth), BF16), pltpu.VMEM((2, seq, wide), BF16),
                pltpu.VMEM((tiles, 4, seq // 8, wide), BF16), pltpu.SemaphoreType.DMA((2,)),
                pltpu.SemaphoreType.DMA((tiles, 4)), pltpu.SemaphoreType.DMA((tiles, 4))]

    @staticmethod
    def out(seq, hid, wide, first):
        last = hid // wide - 1
        spec = pl.BlockSpec((seq // 8, wide), lambda j: (0, jnp.clip(j - first - 1, 0, last)))
        return [spec] * 4, [sds((seq // 8, hid), F32)] + [sds((seq // 8, hid))] * 3


def gelu_pair(a, b):
    tanh = jnp.tanh(GELU_C * (a + GELU_A * a * a * a))
    slope = (0.5 * (1.0 + tanh)
             + 0.5 * a * (1.0 - tanh * tanh) * GELU_C * (1.0 + 3.0 * GELU_A * a * a))
    return (0.5 * a * (1.0 + tanh)).astype(BF16), (b * slope).astype(BF16)


def mlp_kernel(m, nt, h_ref, dy_ref, mu_ref, rs_ref, g_ref, up_ref, down_ref, up_hbm,
               n_hbm, act_ref, dpre_hbm, keep_ref, s1_ref, s2_ref, s3_ref,
               n_v, dy_v, dpre_v, a_v, b_v, h_sem, dy_sem, out_sem, *split_refs):
    step = pl.program_id(0)
    bn = up_ref.shape[1]
    chunks = h_sem.shape[0]
    part = n_v.shape[0] // chunks
    split = Split(dpre_v, up_hbm, (keep_ref, s1_ref, s2_ref, s3_ref), *split_refs)
    n_out = pltpu.make_async_copy(n_v, n_hbm, out_sem.at[0])
    d_out = pltpu.make_async_copy(dpre_v, dpre_hbm, out_sem.at[1])

    def load(r):
        rows = pl.ds(pl.multiple_of(r * part, part), part)
        return (pltpu.make_async_copy(h_ref.at[m, rows], n_v.at[rows], h_sem.at[r]),
                pltpu.make_async_copy(dy_ref.at[m, rows], dy_v.at[rows], dy_sem.at[r]))

    @pl.when(step == 0)
    def _():
        for r in range(chunks):
            for copy in load(r):
                copy.start()
        split.greet()

        @pl.loop(0, chunks)
        def _(r):
            rows = pl.ds(pl.multiple_of(r * part, part), part)
            h_copy, dy_copy = load(r)
            h_copy.wait()
            n_v[rows, :] = normed(n_v[rows, :], mu_ref[m:m + 1, rows], rs_ref[m:m + 1, rows], g_ref[...])
            dy_copy.wait()
            a_v[rows, :] = mm(n_v[rows, :], up_ref[...])
            b_v[rows, :] = mm(dy_v[rows, :], down_ref[...], NT)

        n_out.start()

    def finish():
        act, dpre = gelu_pair(a_v[...], b_v[...])
        act_ref[...] = act
        dpre_v[:, pl.ds(pl.multiple_of((step - 1) * bn, bn), bn)] = dpre

    @pl.when(jnp.logical_and(step > 0, step < nt))
    def _():
        finish()
        a_v[...] = mm(n_v[...], up_ref[...])
        b_v[...] = mm(dy_v[...], down_ref[...], NT)

    @pl.when(step == nt - 2)
    def _():
        split.load(0).start()
        split.load(1).start()

    @pl.when(step == nt)
    def _():
        finish()
        d_out.start()

    @pl.when(step >= nt)
    def _():
        split.tile(step - nt)

    @pl.when(step == nt + split.tiles)
    def _():
        n_out.wait()
        d_out.wait()


def mlp(m, h1, dy, stats, gain, w_up, w_down, token):
    _, seq, hid = h1.shape
    ffn = w_up.shape[1]
    bn, wide, chunks = 256, 1024, 4
    nt, tiles = ffn // bn, hid // wide
    col = lambda j: jnp.minimum(j, nt - 1)
    sum_specs, sums = Split.out(seq, hid, wide, nt)
    return call(
        partial(mlp_kernel, m, nt), (nt + tiles + 1,),
        [ANY, ANY, whole(stats[0]), whole(stats[1]), whole(gain),
         pl.BlockSpec((hid, bn), lambda j: (0, col(j))), pl.BlockSpec((bn, hid), lambda j: (col(j), 0)), ANY],
        [h1, dy, *stats, gain, w_up, w_down, w_up],
        [ANY, pl.BlockSpec((seq, bn), lambda j: (0, jnp.clip(j - 1, 0, nt - 1))), ANY] + sum_specs,
        [sds((seq, hid)), sds((seq, ffn)), sds((seq, ffn))] + sums, token, 6 * seq * hid * ffn,
        scratch=[pltpu.VMEM((seq, hid), BF16), pltpu.VMEM((seq, hid), BF16), pltpu.VMEM((seq, ffn), BF16),
                 pltpu.VMEM((seq, bn), F32), pltpu.VMEM((seq, bn), F32),
                 pltpu.SemaphoreType.DMA((chunks,)), pltpu.SemaphoreType.DMA((chunks,)), pltpu.SemaphoreType.DMA((2,)),
                 *Split.scratch(seq, ffn, hid, wide)],
        name='mlp', cid=m)


def qkv_kernel(m, x_ref, mu_ref, rs_ref, g_ref, w_ref, n_hbm, out_ref, n_v, x_sem, out_sem):
    step = pl.program_id(0)
    chunks = x_sem.shape[0]
    part = n_v.shape[0] // chunks
    n_out = pltpu.make_async_copy(n_v, n_hbm, out_sem)

    def load(r):
        rows = pl.ds(pl.multiple_of(r * part, part), part)
        return pltpu.make_async_copy(x_ref.at[m, rows], n_v.at[rows], x_sem.at[r])

    @pl.when(step == 0)
    def _():
        for r in range(chunks):
            load(r).start()

        @pl.loop(0, chunks)
        def _(r):
            rows = pl.ds(pl.multiple_of(r * part, part), part)
            load(r).wait()
            n_v[rows, :] = normed(n_v[rows, :], mu_ref[m:m + 1, rows], rs_ref[m:m + 1, rows], g_ref[...])
            out_ref[rows, :] = mm(n_v[rows, :], w_ref[...]).astype(BF16)
        n_out.start()

    @pl.when(step > 0)
    def _():
        out_ref[...] = mm(n_v[...], w_ref[...]).astype(BF16)

    @pl.when(step == pl.num_programs(0) - 1)
    def _():
        n_out.wait()


def qkv_proj(m, x, stats, gain, w, token):
    _, seq, hid = x.shape
    bn, chunks = 256, 4
    return call(
        partial(qkv_kernel, m), (w.shape[1] // bn,),
        [ANY, whole(stats[0]), whole(stats[1]), whole(gain),
         pl.BlockSpec((hid, bn), lambda j: (0, j))],
        [x, *stats, gain, w], [ANY, pl.BlockSpec((seq, bn), lambda j: (0, j))],
        [sds((seq, hid)), sds((seq, w.shape[1]))], token, 2 * seq * hid * w.shape[1],
        scratch=[pltpu.VMEM((seq, hid), BF16), pltpu.SemaphoreType.DMA((chunks,)), pltpu.SemaphoreType.DMA],
        name='qkv')


def norm_kernel(m, pos_ref, keep_ref, r1_ref, r2_ref, r3_ref, act_ref, res_ref, mu_ref, rs_ref, g_ref, out_ref,
                mu_v, rs_v):
    blk, hid = keep_ref.shape
    high, wide = 16, 512
    mu_v[...] = jnp.broadcast_to(mu_ref[m:m + 1, :], (128, blk)).T
    rs_v[...] = jnp.broadcast_to(rs_ref[m:m + 1, :], (128, blk)).T

    @pl.loop(0, blk // high)
    def _(i):
        rows = pl.ds(pl.multiple_of(i * high, high), high)
        mean, rstd = mu_v[rows, 0:1], rs_v[rows, 0:1]

        def terms(j):
            cols = pl.ds(j * wide, wide)
            total = (keep_ref[rows, cols] + r1_ref[rows, cols].astype(F32) + r2_ref[rows, cols].astype(F32)
                     + r3_ref[rows, cols].astype(F32))
            hat = (act_ref[0, rows, cols].astype(F32) - mean) * rstd
            return cols, total * g_ref[:, cols].astype(F32), hat

        plain = cross = jnp.zeros((high, wide), F32)
        for j in range(hid // wide):
            _, scaled, hat = terms(j)
            plain = plain + scaled
            cross = cross + scaled * hat
        mean_scaled = jnp.sum(plain, axis=-1, keepdims=True) * (1.0 / hid)
        mean_cross = jnp.sum(cross, axis=-1, keepdims=True) * (1.0 / hid)
        for j in range(hid // wide):
            cols, scaled, hat = terms(j)
            res = (res_ref[0, rows, cols] if len(res_ref.shape) == 3 else res_ref[rows, cols]).astype(F32)
            out_ref[rows, cols] = (res + rstd * (scaled - mean_scaled - hat * mean_cross)).astype(BF16)


def norm_shard(m, keep, got, acts, resid, stats, gain, pos, token):
    blk, hid = keep.shape
    local = pl.BlockSpec((blk, hid), lambda i, p: (0, 0))
    row = pl.BlockSpec((1, blk, hid), lambda i, p: (m, p[0], 0))
    stat = pl.BlockSpec((stats[0].shape[0], blk), lambda i, p: (0, p[0]))
    return call(
        partial(norm_kernel, m), (1,),
        [local] * 4 + [row, row if resid.ndim == 3 else local, stat, stat, whole(gain)],
        [keep, *got, acts, resid, *stats, gain], [local], [sds((blk, hid))], token, 20 * blk * hid,
        scratch=[pltpu.VMEM((blk, 128), F32)] * 2, pos=pos, name='norm')


def head_backward(scale, q_ref, k_ref, v_ref, do_ref, o_ref, dq_ref, dk_ref, dv_ref, dk_acc, dv_acc):
    seq = do_ref.shape[0]
    k_all, v_all = k_ref[...], v_ref[...]
    k_t, v_t = k_all.T, v_all.T
    nblk = seq // BQ
    kpos = lax.broadcasted_iota(jnp.int32, (BQ, BQ), 0)
    qpos = lax.broadcasted_iota(jnp.int32, (BQ, BQ), 1)
    for i in reversed(range(nblk)):
        rows = pl.ds(i * BQ, BQ)
        width = (i + 1) * BQ
        q, do = q_ref[rows, :], do_ref[rows, :]
        s_t = mm(k_all[:width], q, NT)
        last = jnp.where(qpos >= kpos, s_t[i * BQ:], -1e30)
        s_t = jnp.concatenate([s_t[:i * BQ], last], axis=0) if i else last
        top = jnp.max(s_t, axis=0, keepdims=True)
        p_t = jnp.exp((s_t - top) * scale)
        p_t = p_t * (1.0 / jnp.sum(p_t, axis=0, keepdims=True))
        p_b = p_t.astype(BF16)
        o_ref[rows, :] = mm(v_t[:, :width], p_b).T.astype(BF16)
        dp_t = mm(v_all[:width], do, NT)
        dot = jnp.sum(p_t * dp_t, axis=0, keepdims=True)
        ds_t = (p_t * (dp_t - dot) * scale).astype(BF16)
        dq_ref[rows, :] = mm(k_t[:, :width], ds_t).T.astype(BF16)
        dv, dk = mm(p_b, do), mm(ds_t, q)
        if i == nblk - 1:
            dv_acc[...] = dv
            dk_acc[...] = dk
        else:
            dv_acc[:width] += dv
            dk_acc[:width] += dk
    dk_ref[...] = dk_acc[...].astype(BF16)
    dv_ref[...] = dv_acc[...].astype(BF16)


def attn_kernel(scale, n, dh_ref, wo_ref, q_ref, k_ref, v_ref, w_hbm,
                o_ref, dq_ref, dk_ref, dv_ref, keep_ref, s1_ref, s2_ref, s3_ref,
                dh_v, do_v, g_v, dk_acc, dv_acc, dh_sem, *split_refs):
    step = pl.program_id(0)
    seq, dim = q_ref.shape
    chunks = dh_sem.shape[0]
    part = seq // chunks
    split = Split(g_v, w_hbm, (keep_ref, s1_ref, s2_ref, s3_ref), *split_refs)

    def load(r):
        rows = pl.ds(pl.multiple_of(r * part, part), part)
        return pltpu.make_async_copy(dh_ref.at[rows], dh_v.at[rows], dh_sem.at[r])

    @pl.when(step == 0)
    def _():
        for r in range(chunks):
            load(r).start()
        split.greet()

        @pl.loop(0, chunks)
        def _(r):
            rows = pl.ds(pl.multiple_of(r * part, part), part)
            load(r).wait()
            grad_o = mm(dh_v[rows, :], wo_ref[...], NT).astype(BF16)
            for h in range(n):
                do_v[h, rows, :] = grad_o[:, h * dim:(h + 1) * dim]
        split.load(0).start()
        split.load(1).start()

    @pl.when(step < n)
    def _():
        head_backward(scale, q_ref, k_ref, v_ref, do_v.at[step], o_ref, dq_ref, dk_ref, dv_ref, dk_acc, dv_acc)
        for c, ref in enumerate((dq_ref, dk_ref, dv_ref)):
            g_v[:, pl.ds(pl.multiple_of((c * n + step) * dim, dim), dim)] = ref[...]

    @pl.when(step >= n)
    def _():
        split.tile(step - n)


def attention(m, dh, w_out, qkv, w_flat, dim, scale, token):
    seq, hid = dh.shape
    width = w_out.shape[0]
    n = width // dim
    wide, chunks = 1024, 4
    head = lambda c: pl.BlockSpec((seq, dim), lambda i: (0, c * n + jnp.minimum(i, n - 1)))
    sum_specs, sums = Split.out(seq, hid, wide, n)
    return call(
        partial(attn_kernel, scale, n), (n + hid // wide + 1,),
        [ANY, pl.BlockSpec((width, hid), lambda i: (0, 0)), head(0), head(1), head(2), ANY],
        [dh, w_out, qkv, qkv, qkv, w_flat],
        [head(0)] * 4 + sum_specs, [sds((seq, width))] * 4 + sums, token,
        24 * n * seq * seq * dim + 8 * seq * hid * width,
        scratch=[pltpu.VMEM((seq, hid), BF16), pltpu.VMEM((n, seq, dim), BF16), pltpu.VMEM((seq, 3 * width), BF16),
                 pltpu.VMEM((seq, dim), F32), pltpu.VMEM((seq, dim), F32), pltpu.SemaphoreType.DMA((chunks,)),
                 *Split.scratch(seq, 3 * width, hid, wide)],
        name='attn', cid=2 + m)


def copy_kernel(m, src, old, dst, buf, in_sem, out_sem):
    parts = in_sem.shape[0]
    part = src.shape[0] // parts
    at = [pl.ds(r * part, part) for r in range(parts)]
    loads = [pltpu.make_async_copy(src.at[at[r]], buf.at[at[r]], in_sem.at[r]) for r in range(parts)]
    stores = [pltpu.make_async_copy(buf.at[at[r]], dst.at[m, at[r]], out_sem.at[r]) for r in range(parts)]
    for load in loads:
        load.start()
    for load, store in zip(loads, stores):
        load.wait()
        store.start()
    for store in stores:
        store.wait()


def write_out(m, src, old, token):
    parts = 8
    return call(partial(copy_kernel, m), (1,), [ANY, ANY], [src, old], [ANY], [sds(old.shape)], token, src.size,
                scratch=[pltpu.VMEM(src.shape, BF16), pltpu.SemaphoreType.DMA((parts,)),
                         pltpu.SemaphoreType.DMA((parts,))], alias={1: 0}, name='copy')


def grad_kernel(a0_ref, a1_ref, b0_ref, b1_ref, out_ref):
    left = lambda ref: ref[0] if len(ref.shape) == 3 else ref[...]
    acc = mm(left(a0_ref), left(b0_ref), TN) + mm(left(a1_ref), left(b1_ref), TN)
    out_ref[...] = acc.astype(BF16)


def weight_grad(lhs, rhs, token, ba, bb, name):
    def split(v, size, axis):
        if isinstance(v, (list, tuple)):
            spec = pl.BlockSpec((v[0].shape[0], size), lambda i, j: (0, (i, j)[axis]))
            return list(v), [spec] * 2, v[0].shape
        specs = [pl.BlockSpec((1, v.shape[1], size), lambda i, j, m=m: (m, 0, (i, j)[axis])) for m in range(2)]
        return [v, v], specs, v.shape[1:]

    la, ls, (seq, wa) = split(lhs, ba, 0)
    ra, rs, (_, wb) = split(rhs, bb, 1)
    return call(grad_kernel, (wa // ba, wb // bb), ls + rs, la + ra, [pl.BlockSpec((ba, bb), lambda i, j: (i, j))],
                [sds((wa, wb))], token, 4 * seq * wa * wb, name=name)


def qkv_grad_kernel(a0_ref, a1_ref, *refs):
    src, out_ref, dst, buf, in_sem, out_sem = refs[6], *refs[7:]
    rows, _, heads, dim = out_ref.shape
    step, steps = pl.program_id(0), pl.num_programs(0)
    part = src.shape[0] // in_sem.shape[0]

    def move(r, out):
        at = pl.ds(r * part, part)
        if out:
            return pltpu.make_async_copy(buf.at[at], dst.at[0, at], out_sem.at[r])
        return pltpu.make_async_copy(src.at[at], buf.at[at], in_sem.at[r])

    for r in range(in_sem.shape[0]):
        @pl.when(step == r)
        def _():
            move(r, False).start()

        @pl.when(step == r + 1)
        def _():
            move(r, False).wait()
            move(r, True).start()

    for c in range(3):
        acc = mm(a0_ref[...], refs[c][...], TN) + mm(a1_ref[...], refs[3 + c][...], TN)
        out_ref[:, c] = acc.reshape(rows, heads, dim).astype(BF16)

    @pl.when(step == steps - 1)
    def _():
        for r in range(in_sem.shape[0]):
            move(r, True).wait()


def qkv_grad(norms, grads, heads, dim, dx, count, token):
    seq, hid = norms[0].shape
    ba, parts = 512, 4
    lhs = pl.BlockSpec((seq, ba), lambda i: (0, i))
    rhs = pl.BlockSpec((seq, heads * dim), lambda i: (0, 0))
    return call(qkv_grad_kernel, (hid // ba,), [lhs] * 2 + [rhs] * 6 + [ANY], [*norms, *grads[0], *grads[1], dx],
                [pl.BlockSpec((ba, 3, heads, dim), lambda i: (i, 0, 0, 0)), ANY],
                [sds((hid, 3, heads, dim)), sds((count, *dx.shape))], token, 12 * seq * hid * heads * dim,
                scratch=[pltpu.VMEM(dx.shape, BF16), pltpu.SemaphoreType.DMA((parts,)),
                         pltpu.SemaphoreType.DMA((parts,))], name='dqkvw')


def flat_kernel(w_ref, out_ref):
    rows, _, heads, dim = w_ref.shape
    for c in range(3):
        out_ref[:, pl.ds(c * heads * dim, heads * dim)] = w_ref[:, c].reshape(rows, heads * dim)


def flat_weight(w, token):
    hid, three, heads, dim = w.shape
    bm = 1024
    return call(flat_kernel, (hid // bm,), [pl.BlockSpec((bm, three, heads, dim), lambda i: (i, 0, 0, 0))], [w],
                [pl.BlockSpec((bm, three * heads * dim), lambda i: (i, 0))], [sds((hid, three * heads * dim))], token,
                w.size, name='flat')


def swap(arr, bit):
    return lax.ppermute(arr, 'tp', [(i, i ^ bit) for i in range(8)])


def solution(mesh):
    act_spec = P('dp', None, None)
    stat_spec = P('dp', None)
    in_specs = (act_spec, act_spec, act_spec, stat_spec, stat_spec, stat_spec, stat_spec, P(), P(),
                P(None, 'tp', None, None), P('tp', None, None), P(None, 'tp'), P('tp', None))
    out_specs = (act_spec, P('dp', 'tp', None, None), P(('dp', 'tp'), None, None), P('dp', 'tp'),
                 P(('dp', 'tp'), None))

    def local_backward(x_saved, h1_saved, grad_y, mean_one, rstd_one, mean_two, rstd_two,
                       gain_one, gain_two, w_qkv, w_out, w_up, w_down):
        hid, heads, _, dim = w_qkv.shape
        scale = dim ** -0.5
        idx = lax.axis_index('tp')
        pos = jnp.stack([idx, idx // 2, idx % 2]).astype(jnp.int32)
        stats_one, stats_two = (mean_one, rstd_one), (mean_two, rstd_two)
        g1, g2 = gain_one.reshape(1, hid), gain_two.reshape(1, hid)
        w_out = w_out.reshape(heads * dim, hid)
        tok = jnp.zeros((8, 128), F32)

        def gather(shard):
            return lax.all_gather(shard, 'tp', axis=0, tiled=True)

        def exchange(sends):
            return [swap(s, bit) for s, bit in zip(sends, (2, 4, 6))]

        n2, act, dpre, n1, qkv = [0, 0], [0, 0], [0, 0], [0, 0], [0, 0]
        dh_shard, dh, out, grads, dx = [0, 0], [0, 0], [0, 0], [0, 0], [0, 0]

        n2[0], act[0], dpre[0], keep_a, *send, tok = mlp(0, h1_saved, grad_y, stats_two, g2, w_up, w_down, tok)
        got_a = exchange(send)
        n2[1], act[1], dpre[1], keep_b, *send, tok = mlp(1, h1_saved, grad_y, stats_two, g2, w_up, w_down, tok)
        got_b = exchange(send)
        dh_shard[0], tok = norm_shard(0, keep_a, got_a, h1_saved, grad_y, stats_two, g2, pos, tok)
        dh[0] = gather(dh_shard[0])
        w_flat, tok = flat_weight(w_qkv.transpose(0, 2, 1, 3), tok)
        n1[0], qkv[0], tok = qkv_proj(0, x_saved, stats_one, g1, w_flat, tok)
        n1[1], qkv[1], tok = qkv_proj(1, x_saved, stats_one, g1, w_flat, tok)
        dh_shard[1], tok = norm_shard(1, keep_b, got_b, h1_saved, grad_y, stats_two, g2, pos, tok)
        dh[1] = gather(dh_shard[1])

        out[0], *g0, keep_a, s1, s2, s3, tok = attention(0, dh[0], w_out, qkv[0], w_flat, dim, scale, tok)
        got_a = exchange((s1, s2, s3))
        out[1], *g1s, keep_b, s1, s2, s3, tok = attention(1, dh[1], w_out, qkv[1], w_flat, dim, scale, tok)
        got_b = exchange((s1, s2, s3))
        dx_shard, tok = norm_shard(0, keep_a, got_a, x_saved, dh_shard[0], stats_one, g1, pos, tok)
        dx[0] = gather(dx_shard)
        grad_down, tok = weight_grad(act, grad_y, tok, 1024, 1024, 'dw2')
        grad_up, tok = weight_grad(n2, dpre, tok, 1024, 1024, 'dw1')
        dx_shard, tok = norm_shard(1, keep_b, got_b, x_saved, dh_shard[1], stats_one, g1, pos, tok)
        dx[1] = gather(dx_shard)
        grad_out_w, tok = weight_grad(out, dh, tok, 512, 1024, 'dwo')
        grad_qkv_w, grad_x, tok = qkv_grad(n1, [g0, g1s], heads, dim, dx[0], 2, tok)
        grad_x, tok = write_out(1, dx[1], grad_x, tok)
        return grad_x, grad_qkv_w.transpose(0, 2, 1, 3), grad_out_w.reshape(heads, dim, hid), grad_up, grad_down

    return jax.shard_map(local_backward, mesh=mesh, in_specs=in_specs, out_specs=out_specs, check_vma=False)
```

```python
import jax
import jax.numpy as jnp
from jax import lax
from jax.sharding import PartitionSpec as P
from jax.experimental import pallas as pl
from jax.experimental.pallas import tpu as pltpu
from functools import partial

GELU_C = 0.7978845608028654
GELU_A = 0.044715
F32 = jnp.float32
BF16 = jnp.bfloat16
BQ = 256
NT = (((1,), (1,)), ((), ()))
TN = (((0,), (0,)), ((), ()))
ANY = pl.BlockSpec(memory_space=pl.ANY)
TOKEN = jax.ShapeDtypeStruct((8, 128), F32)


def mm(a, b, dims=(((1,), (0,)), ((), ()))):
    return lax.dot_general(a, b, dims, preferred_element_type=F32)


def call(body, grid, in_specs, args, out_specs, outs, token, flops, scratch=(), pos=None, name=None, alias=None, cid=None):
    n_in, n_out, n_pos = len(args), len(outs), 0 if pos is None else 1

    def kernel(*refs):
        head, refs = refs[:n_pos], refs[n_pos:]
        body(*head, *refs[:n_in], *refs[n_in + 1:n_in + 1 + n_out], *refs[n_in + 2 + n_out:])

    size = sum(o.size * o.dtype.itemsize for o in outs) + sum(a.size * a.dtype.itemsize for a in args)
    results = pl.pallas_call(
        kernel,
        grid_spec=pltpu.PrefetchScalarGridSpec(
            num_scalar_prefetch=n_pos, grid=grid, in_specs=list(in_specs) + [ANY],
            out_specs=list(out_specs) + [ANY], scratch_shapes=list(scratch)),
        out_shape=list(outs) + [TOKEN],
        compiler_params=pltpu.CompilerParams(vmem_limit_bytes=62 * 1024 * 1024, collective_id=cid, has_side_effects=cid is not None),
        cost_estimate=pl.CostEstimate(flops=int(flops), bytes_accessed=int(size), transcendentals=0),
        input_output_aliases=alias or {},
        name=name,
    )(*([] if pos is None else [pos]), *args, token)
    return results


def whole(arr):
    return pl.BlockSpec(arr.shape, lambda *ids: (0,) * arr.ndim)


def sds(shape, dtype=BF16):
    return jax.ShapeDtypeStruct(shape, dtype)


def column(row):
    return jnp.broadcast_to(row, (8, row.shape[1])).T[:, 0:1]


def normed(rows, mean, rstd, gain):
    return ((rows.astype(F32) - column(mean)) * column(rstd) * gain.astype(F32)).astype(BF16)


class Split:
    def __init__(self, lhs, w_hbm, outs, wrow, prod, got, w_sem, send_sem, recv_sem):
        self.lhs, self.w_hbm, self.outs = lhs, w_hbm, outs
        self.wrow, self.prod, self.got = wrow, prod, got
        self.w_sem, self.send_sem, self.recv_sem = w_sem, send_sem, recv_sem
        self.wide = wrow.shape[1]
        self.tiles = w_hbm.shape[0] // self.wide
        self.blk = prod.shape[1] // 8
        idx = lax.axis_index('tp')
        self.chip, self.core = lax.div(idx, 2), lax.rem(idx, 2)
        self.partner = 2 * self.chip + 1 - self.core

    def load(self, t):
        return pltpu.make_async_copy(self.w_hbm.at[pl.ds(t * self.wide, self.wide), :], self.wrow.at[t % 2],
                                     self.w_sem.at[t % 2])

    def rows(self, k, core):
        return pl.ds(pl.multiple_of((2 * lax.bitwise_xor(self.chip, k) + core) * self.blk, self.blk), self.blk)

    def send(self, t, k):
        return pltpu.make_async_remote_copy(
            src_ref=self.prod.at[t % 2, self.rows(k, 1 - self.core)], dst_ref=self.got.at[t, k],
            send_sem=self.send_sem.at[t, k], recv_sem=self.recv_sem.at[t, k],
            device_id={'tp': self.partner}, device_id_type=pl.DeviceIdType.MESH)

    def greet(self):
        barrier = pltpu.get_barrier_semaphore()
        pl.semaphore_signal(barrier, inc=1, device_id={'tp': self.partner}, device_id_type=pl.DeviceIdType.MESH)
        pl.semaphore_wait(barrier, 1)

    def tile(self, t):
        @pl.when(t < self.tiles)
        def _():
            self.load(t).wait()

            @pl.when(t >= 2)
            def _():
                for k in range(4):
                    self.send(t - 2, k).wait_send()

            self.prod[t % 2] = mm(self.lhs[...], self.wrow[t % 2], NT).astype(BF16)
            for k in range(4):
                self.send(t, k).start()

            @pl.when(t + 2 < self.tiles)
            def _():
                self.load(t + 2).start()

        @pl.when(t > 0)
        def _():
            for k in range(4):
                self.send(t - 1, k).wait_recv()
                total = self.prod[(t - 1) % 2, self.rows(k, self.core)].astype(F32) + self.got[t - 1, k].astype(F32)
                self.outs[k][...] = total.astype(self.outs[k].dtype)

        @pl.when(t == self.tiles)
        def _():
            for u in range(self.tiles - 2, self.tiles):
                for k in range(4):
                    self.send(u, k).wait_send()

    @staticmethod
    def scratch(seq, depth, hid, wide):
        tiles = hid // wide
        return [pltpu.VMEM((2, wide, depth), BF16), pltpu.VMEM((2, seq, wide), BF16),
                pltpu.VMEM((tiles, 4, seq // 8, wide), BF16), pltpu.SemaphoreType.DMA((2,)),
                pltpu.SemaphoreType.DMA((tiles, 4)), pltpu.SemaphoreType.DMA((tiles, 4))]

    @staticmethod
    def out(seq, hid, wide, first):
        last = hid // wide - 1
        spec = pl.BlockSpec((seq // 8, wide), lambda j: (0, jnp.clip(j - first - 1, 0, last)))
        return [spec] * 4, [sds((seq // 8, hid), F32)] + [sds((seq // 8, hid))] * 3


def gelu_pair(a, b):
    tanh = jnp.tanh(GELU_C * (a + GELU_A * a * a * a))
    slope = (0.5 * (1.0 + tanh)
             + 0.5 * a * (1.0 - tanh * tanh) * GELU_C * (1.0 + 3.0 * GELU_A * a * a))
    return (0.5 * a * (1.0 + tanh)).astype(BF16), (b * slope).astype(BF16)


def mlp_kernel(m, nt, h_ref, dy_ref, mu_ref, rs_ref, g_ref, up_ref, down_ref, up_hbm,
               n_hbm, act_ref, dpre_hbm, keep_ref, s1_ref, s2_ref, s3_ref,
               n_v, dy_v, dpre_v, a_v, b_v, h_sem, dy_sem, out_sem, *split_refs):
    step = pl.program_id(0)
    bn = up_ref.shape[1]
    chunks = h_sem.shape[0]
    part = n_v.shape[0] // chunks
    split = Split(dpre_v, up_hbm, (keep_ref, s1_ref, s2_ref, s3_ref), *split_refs)
    n_out = pltpu.make_async_copy(n_v, n_hbm, out_sem.at[0])
    d_out = pltpu.make_async_copy(dpre_v, dpre_hbm, out_sem.at[1])

    def load(r):
        rows = pl.ds(pl.multiple_of(r * part, part), part)
        return (pltpu.make_async_copy(h_ref.at[m, rows], n_v.at[rows], h_sem.at[r]),
                pltpu.make_async_copy(dy_ref.at[m, rows], dy_v.at[rows], dy_sem.at[r]))

    @pl.when(step == 0)
    def _():
        for r in range(chunks):
            for copy in load(r):
                copy.start()
        split.greet()

        @pl.loop(0, chunks)
        def _(r):
            rows = pl.ds(pl.multiple_of(r * part, part), part)
            h_copy, dy_copy = load(r)
            h_copy.wait()
            dy_copy.wait()
            b_v[rows, :] = mm(dy_v[rows, :], down_ref[...], NT)
            hat = normed(n_v[rows, :], mu_ref[m:m + 1, rows], rs_ref[m:m + 1, rows], g_ref[...])
            n_v[rows, :] = hat
            a_v[rows, :] = mm(hat, up_ref[...])

        n_out.start()

    def finish():
        act, dpre = gelu_pair(a_v[...], b_v[...])
        act_ref[...] = act
        dpre_v[:, pl.ds(pl.multiple_of((step - 1) * bn, bn), bn)] = dpre

    @pl.when(jnp.logical_and(step > 0, step < nt))
    def _():
        finish()
        a_v[...] = mm(n_v[...], up_ref[...])
        b_v[...] = mm(dy_v[...], down_ref[...], NT)

    @pl.when(step == nt - 2)
    def _():
        split.load(0).start()
        split.load(1).start()

    @pl.when(step == nt)
    def _():
        finish()
        d_out.start()

    @pl.when(step >= nt)
    def _():
        split.tile(step - nt)

    @pl.when(step == nt + split.tiles)
    def _():
        n_out.wait()
        d_out.wait()


def mlp(m, h1, dy, stats, gain, w_up, w_down, token):
    _, seq, hid = h1.shape
    ffn = w_up.shape[1]
    bn, wide, chunks = 256, 1024, 4
    nt, tiles = ffn // bn, hid // wide
    col = lambda j: jnp.minimum(j, nt - 1)
    sum_specs, sums = Split.out(seq, hid, wide, nt)
    return call(
        partial(mlp_kernel, m, nt), (nt + tiles + 1,),
        [ANY, ANY, whole(stats[0]), whole(stats[1]), whole(gain),
         pl.BlockSpec((hid, bn), lambda j: (0, col(j))), pl.BlockSpec((bn, hid), lambda j: (col(j), 0)), ANY],
        [h1, dy, *stats, gain, w_up, w_down, w_up],
        [ANY, pl.BlockSpec((seq, bn), lambda j: (0, jnp.clip(j - 1, 0, nt - 1))), ANY] + sum_specs,
        [sds((seq, hid)), sds((seq, ffn)), sds((seq, ffn))] + sums, token, 6 * seq * hid * ffn,
        scratch=[pltpu.VMEM((seq, hid), BF16), pltpu.VMEM((seq, hid), BF16), pltpu.VMEM((seq, ffn), BF16),
                 pltpu.VMEM((seq, bn), F32), pltpu.VMEM((seq, bn), F32),
                 pltpu.SemaphoreType.DMA((chunks,)), pltpu.SemaphoreType.DMA((chunks,)), pltpu.SemaphoreType.DMA((2,)),
                 *Split.scratch(seq, ffn, hid, wide)],
        name='mlp', cid=m)


def qkv_kernel(m, x_ref, mu_ref, rs_ref, g_ref, w_ref, n_hbm, out_ref, n_v, x_sem, out_sem):
    step = pl.program_id(0)
    chunks = x_sem.shape[0]
    part = n_v.shape[0] // chunks
    n_out = pltpu.make_async_copy(n_v, n_hbm, out_sem)

    def load(r):
        rows = pl.ds(pl.multiple_of(r * part, part), part)
        return pltpu.make_async_copy(x_ref.at[m, rows], n_v.at[rows], x_sem.at[r])

    @pl.when(step == 0)
    def _():
        for r in range(chunks):
            load(r).start()

        @pl.loop(0, chunks)
        def _(r):
            rows = pl.ds(pl.multiple_of(r * part, part), part)
            load(r).wait()
            n_v[rows, :] = normed(n_v[rows, :], mu_ref[m:m + 1, rows], rs_ref[m:m + 1, rows], g_ref[...])
            out_ref[rows, :] = mm(n_v[rows, :], w_ref[...]).astype(BF16)
        n_out.start()

    @pl.when(step > 0)
    def _():
        out_ref[...] = mm(n_v[...], w_ref[...]).astype(BF16)

    @pl.when(step == pl.num_programs(0) - 1)
    def _():
        n_out.wait()


def qkv_proj(m, x, stats, gain, w, token):
    _, seq, hid = x.shape
    bn, chunks = 256, 4
    return call(
        partial(qkv_kernel, m), (w.shape[1] // bn,),
        [ANY, whole(stats[0]), whole(stats[1]), whole(gain),
         pl.BlockSpec((hid, bn), lambda j: (0, j))],
        [x, *stats, gain, w], [ANY, pl.BlockSpec((seq, bn), lambda j: (0, j))],
        [sds((seq, hid)), sds((seq, w.shape[1]))], token, 2 * seq * hid * w.shape[1],
        scratch=[pltpu.VMEM((seq, hid), BF16), pltpu.SemaphoreType.DMA((chunks,)), pltpu.SemaphoreType.DMA],
        name='qkv')


def norm_kernel(m, pos_ref, keep_ref, r1_ref, r2_ref, r3_ref, act_ref, res_ref, mu_ref, rs_ref, g_ref, out_ref,
                mu_v, rs_v):
    blk, hid = keep_ref.shape
    high, wide = 16, 512
    mu_v[...] = jnp.broadcast_to(mu_ref[m:m + 1, :], (128, blk)).T
    rs_v[...] = jnp.broadcast_to(rs_ref[m:m + 1, :], (128, blk)).T

    @pl.loop(0, blk // high)
    def _(i):
        rows = pl.ds(pl.multiple_of(i * high, high), high)
        mean, rstd = mu_v[rows, 0:1], rs_v[rows, 0:1]

        def terms(j):
            cols = pl.ds(j * wide, wide)
            total = (keep_ref[rows, cols] + r1_ref[rows, cols].astype(F32) + r2_ref[rows, cols].astype(F32)
                     + r3_ref[rows, cols].astype(F32))
            hat = (act_ref[0, rows, cols].astype(F32) - mean) * rstd
            return cols, total * g_ref[:, cols].astype(F32), hat

        plain = cross = jnp.zeros((high, wide), F32)
        for j in range(hid // wide):
            _, scaled, hat = terms(j)
            plain = plain + scaled
            cross = cross + scaled * hat
        mean_scaled = jnp.sum(plain, axis=-1, keepdims=True) * (1.0 / hid)
        mean_cross = jnp.sum(cross, axis=-1, keepdims=True) * (1.0 / hid)
        for j in range(hid // wide):
            cols, scaled, hat = terms(j)
            res = (res_ref[0, rows, cols] if len(res_ref.shape) == 3 else res_ref[rows, cols]).astype(F32)
            out_ref[rows, cols] = (res + rstd * (scaled - mean_scaled - hat * mean_cross)).astype(BF16)


def norm_shard(m, keep, got, acts, resid, stats, gain, pos, token):
    blk, hid = keep.shape
    local = pl.BlockSpec((blk, hid), lambda i, p: (0, 0))
    row = pl.BlockSpec((1, blk, hid), lambda i, p: (m, p[0], 0))
    stat = pl.BlockSpec((stats[0].shape[0], blk), lambda i, p: (0, p[0]))
    return call(
        partial(norm_kernel, m), (1,),
        [local] * 4 + [row, row if resid.ndim == 3 else local, stat, stat, whole(gain)],
        [keep, *got, acts, resid, *stats, gain], [local], [sds((blk, hid))], token, 20 * blk * hid,
        scratch=[pltpu.VMEM((blk, 128), F32)] * 2, pos=pos, name='norm')


def head_backward(scale, q_ref, k_ref, v_ref, do_ref, o_ref, dq_ref, dk_ref, dv_ref, dk_acc, dv_acc):
    seq = do_ref.shape[0]
    k_all, v_all = k_ref[...], v_ref[...]
    k_t, v_t = k_all.T, v_all.T
    nblk = seq // BQ
    kpos = lax.broadcasted_iota(jnp.int32, (BQ, BQ), 0)
    qpos = lax.broadcasted_iota(jnp.int32, (BQ, BQ), 1)
    for i in reversed(range(nblk)):
        rows = pl.ds(i * BQ, BQ)
        width = (i + 1) * BQ
        q, do = q_ref[rows, :], do_ref[rows, :]
        s_t = mm(k_all[:width], q, NT)
        last = jnp.where(qpos >= kpos, s_t[i * BQ:], -1e30)
        s_t = jnp.concatenate([s_t[:i * BQ], last], axis=0) if i else last
        top = jnp.max(s_t, axis=0, keepdims=True)
        p_t = jnp.exp((s_t - top) * scale)
        p_t = p_t * (1.0 / jnp.sum(p_t, axis=0, keepdims=True))
        p_b = p_t.astype(BF16)
        o_ref[rows, :] = mm(v_t[:, :width], p_b).T.astype(BF16)
        dp_t = mm(v_all[:width], do, NT)
        dot = jnp.sum(p_t * dp_t, axis=0, keepdims=True)
        ds_t = (p_t * (dp_t - dot) * scale).astype(BF16)
        dq_ref[rows, :] = mm(k_t[:, :width], ds_t).T.astype(BF16)
        dv, dk = mm(p_b, do), mm(ds_t, q)
        if i == nblk - 1:
            dv_acc[...] = dv
            dk_acc[...] = dk
        else:
            dv_acc[:width] += dv
            dk_acc[:width] += dk
    dk_ref[...] = dk_acc[...].astype(BF16)
    dv_ref[...] = dv_acc[...].astype(BF16)


def attn_kernel(scale, n, dh_ref, wo_ref, q_ref, k_ref, v_ref, w_hbm,
                o_ref, dq_ref, dk_ref, dv_ref, keep_ref, s1_ref, s2_ref, s3_ref,
                dh_v, do_v, g_v, dk_acc, dv_acc, dh_sem, *split_refs):
    step = pl.program_id(0)
    seq, dim = q_ref.shape
    chunks = dh_sem.shape[0]
    part = seq // chunks
    split = Split(g_v, w_hbm, (keep_ref, s1_ref, s2_ref, s3_ref), *split_refs)

    def load(r):
        rows = pl.ds(pl.multiple_of(r * part, part), part)
        return pltpu.make_async_copy(dh_ref.at[rows], dh_v.at[rows], dh_sem.at[r])

    @pl.when(step == 0)
    def _():
        for r in range(chunks):
            load(r).start()
        split.greet()

        @pl.loop(0, chunks)
        def _(r):
            rows = pl.ds(pl.multiple_of(r * part, part), part)
            load(r).wait()
            grad_o = mm(dh_v[rows, :], wo_ref[...], NT).astype(BF16)
            for h in range(n):
                do_v[h, rows, :] = grad_o[:, h * dim:(h + 1) * dim]
        split.load(0).start()
        split.load(1).start()

    @pl.when(step < n)
    def _():
        head_backward(scale, q_ref, k_ref, v_ref, do_v.at[step], o_ref, dq_ref, dk_ref, dv_ref, dk_acc, dv_acc)
        for c, ref in enumerate((dq_ref, dk_ref, dv_ref)):
            g_v[:, pl.ds(pl.multiple_of((c * n + step) * dim, dim), dim)] = ref[...]

    @pl.when(step >= n)
    def _():
        split.tile(step - n)


def attention(m, dh, w_out, qkv, w_flat, dim, scale, token):
    seq, hid = dh.shape
    width = w_out.shape[0]
    n = width // dim
    wide, chunks = 1024, 4
    head = lambda c: pl.BlockSpec((seq, dim), lambda i: (0, c * n + jnp.minimum(i, n - 1)))
    sum_specs, sums = Split.out(seq, hid, wide, n)
    return call(
        partial(attn_kernel, scale, n), (n + hid // wide + 1,),
        [ANY, pl.BlockSpec((width, hid), lambda i: (0, 0)), head(0), head(1), head(2), ANY],
        [dh, w_out, qkv, qkv, qkv, w_flat],
        [head(0)] * 4 + sum_specs, [sds((seq, width))] * 4 + sums, token,
        24 * n * seq * seq * dim + 8 * seq * hid * width,
        scratch=[pltpu.VMEM((seq, hid), BF16), pltpu.VMEM((n, seq, dim), BF16), pltpu.VMEM((seq, 3 * width), BF16),
                 pltpu.VMEM((seq, dim), F32), pltpu.VMEM((seq, dim), F32), pltpu.SemaphoreType.DMA((chunks,)),
                 *Split.scratch(seq, 3 * width, hid, wide)],
        name='attn', cid=2 + m)


def copy_kernel(m, src, old, dst, buf, in_sem, out_sem):
    parts = in_sem.shape[0]
    part = src.shape[0] // parts
    at = [pl.ds(r * part, part) for r in range(parts)]
    loads = [pltpu.make_async_copy(src.at[at[r]], buf.at[at[r]], in_sem.at[r]) for r in range(parts)]
    stores = [pltpu.make_async_copy(buf.at[at[r]], dst.at[m, at[r]], out_sem.at[r]) for r in range(parts)]
    for load in loads:
        load.start()
    for load, store in zip(loads, stores):
        load.wait()
        store.start()
    for store in stores:
        store.wait()


def write_out(m, src, old, token):
    parts = 8
    return call(partial(copy_kernel, m), (1,), [ANY, ANY], [src, old], [ANY], [sds(old.shape)], token, src.size,
                scratch=[pltpu.VMEM(src.shape, BF16), pltpu.SemaphoreType.DMA((parts,)),
                         pltpu.SemaphoreType.DMA((parts,))], alias={1: 0}, name='copy')


def grad_kernel(a0_ref, a1_ref, b0_ref, b1_ref, out_ref):
    left = lambda ref: ref[0] if len(ref.shape) == 3 else ref[...]
    acc = mm(left(a0_ref), left(b0_ref), TN) + mm(left(a1_ref), left(b1_ref), TN)
    out_ref[...] = acc.astype(BF16)


def weight_grad(lhs, rhs, token, ba, bb, name):
    def split(v, size, axis):
        if isinstance(v, (list, tuple)):
            spec = pl.BlockSpec((v[0].shape[0], size), lambda i, j: (0, (i, j)[axis]))
            return list(v), [spec] * 2, v[0].shape
        specs = [pl.BlockSpec((1, v.shape[1], size), lambda i, j, m=m: (m, 0, (i, j)[axis])) for m in range(2)]
        return [v, v], specs, v.shape[1:]

    la, ls, (seq, wa) = split(lhs, ba, 0)
    ra, rs, (_, wb) = split(rhs, bb, 1)
    return call(grad_kernel, (wa // ba, wb // bb), ls + rs, la + ra, [pl.BlockSpec((ba, bb), lambda i, j: (i, j))],
                [sds((wa, wb))], token, 4 * seq * wa * wb, name=name)


def qkv_grad_kernel(a0_ref, a1_ref, *refs):
    src, out_ref, dst, buf, in_sem, out_sem = refs[6], *refs[7:]
    rows, _, heads, dim = out_ref.shape
    step, steps = pl.program_id(0), pl.num_programs(0)
    part = src.shape[0] // in_sem.shape[0]

    def move(r, out):
        at = pl.ds(r * part, part)
        if out:
            return pltpu.make_async_copy(buf.at[at], dst.at[0, at], out_sem.at[r])
        return pltpu.make_async_copy(src.at[at], buf.at[at], in_sem.at[r])

    for r in range(in_sem.shape[0]):
        @pl.when(step == r)
        def _():
            move(r, False).start()

        @pl.when(step == r + 1)
        def _():
            move(r, False).wait()
            move(r, True).start()

    for c in range(3):
        acc = mm(a0_ref[...], refs[c][...], TN) + mm(a1_ref[...], refs[3 + c][...], TN)
        out_ref[:, c] = acc.reshape(rows, heads, dim).astype(BF16)

    @pl.when(step == steps - 1)
    def _():
        for r in range(in_sem.shape[0]):
            move(r, True).wait()


def qkv_grad(norms, grads, heads, dim, dx, count, token):
    seq, hid = norms[0].shape
    ba, parts = 512, 4
    lhs = pl.BlockSpec((seq, ba), lambda i: (0, i))
    rhs = pl.BlockSpec((seq, heads * dim), lambda i: (0, 0))
    return call(qkv_grad_kernel, (hid // ba,), [lhs] * 2 + [rhs] * 6 + [ANY], [*norms, *grads[0], *grads[1], dx],
                [pl.BlockSpec((ba, 3, heads, dim), lambda i: (i, 0, 0, 0)), ANY],
                [sds((hid, 3, heads, dim)), sds((count, *dx.shape))], token, 12 * seq * hid * heads * dim,
                scratch=[pltpu.VMEM(dx.shape, BF16), pltpu.SemaphoreType.DMA((parts,)),
                         pltpu.SemaphoreType.DMA((parts,))], name='dqkvw')


def flat_kernel(w_ref, out_ref):
    rows, _, heads, dim = w_ref.shape
    for c in range(3):
        out_ref[:, pl.ds(c * heads * dim, heads * dim)] = w_ref[:, c].reshape(rows, heads * dim)


def flat_weight(w, token):
    hid, three, heads, dim = w.shape
    bm = 1024
    return call(flat_kernel, (hid // bm,), [pl.BlockSpec((bm, three, heads, dim), lambda i: (i, 0, 0, 0))], [w],
                [pl.BlockSpec((bm, three * heads * dim), lambda i: (i, 0))], [sds((hid, three * heads * dim))], token,
                w.size, name='flat')


def swap(arr, bit):
    return lax.ppermute(arr, 'tp', [(i, i ^ bit) for i in range(8)])


def solution(mesh):
    act_spec = P('dp', None, None)
    stat_spec = P('dp', None)
    in_specs = (act_spec, act_spec, act_spec, stat_spec, stat_spec, stat_spec, stat_spec, P(), P(),
                P(None, 'tp', None, None), P('tp', None, None), P(None, 'tp'), P('tp', None))
    out_specs = (act_spec, P('dp', 'tp', None, None), P(('dp', 'tp'), None, None), P('dp', 'tp'),
                 P(('dp', 'tp'), None))

    def local_backward(x_saved, h1_saved, grad_y, mean_one, rstd_one, mean_two, rstd_two,
                       gain_one, gain_two, w_qkv, w_out, w_up, w_down):
        hid, heads, _, dim = w_qkv.shape
        scale = dim ** -0.5
        idx = lax.axis_index('tp')
        pos = jnp.stack([idx, idx // 2, idx % 2]).astype(jnp.int32)
        stats_one, stats_two = (mean_one, rstd_one), (mean_two, rstd_two)
        g1, g2 = gain_one.reshape(1, hid), gain_two.reshape(1, hid)
        w_out = w_out.reshape(heads * dim, hid)
        tok = jnp.zeros((8, 128), F32)

        def gather(shard):
            return lax.all_gather(shard, 'tp', axis=0, tiled=True)

        def exchange(sends):
            return [swap(s, bit) for s, bit in zip(sends, (2, 4, 6))]

        n2, act, dpre, n1, qkv = [0, 0], [0, 0], [0, 0], [0, 0], [0, 0]
        dh_shard, dh, out, grads, dx = [0, 0], [0, 0], [0, 0], [0, 0], [0, 0]

        n2[0], act[0], dpre[0], keep_a, *send, tok = mlp(0, h1_saved, grad_y, stats_two, g2, w_up, w_down, tok)
        got_a = exchange(send)
        n2[1], act[1], dpre[1], keep_b, *send, tok = mlp(1, h1_saved, grad_y, stats_two, g2, w_up, w_down, tok)
        got_b = exchange(send)
        dh_shard[0], tok = norm_shard(0, keep_a, got_a, h1_saved, grad_y, stats_two, g2, pos, tok)
        dh[0] = gather(dh_shard[0])
        w_flat, tok = flat_weight(w_qkv.transpose(0, 2, 1, 3), tok)
        n1[0], qkv[0], tok = qkv_proj(0, x_saved, stats_one, g1, w_flat, tok)
        n1[1], qkv[1], tok = qkv_proj(1, x_saved, stats_one, g1, w_flat, tok)
        dh_shard[1], tok = norm_shard(1, keep_b, got_b, h1_saved, grad_y, stats_two, g2, pos, tok)
        dh[1] = gather(dh_shard[1])

        out[0], *g0, keep_a, s1, s2, s3, tok = attention(0, dh[0], w_out, qkv[0], w_flat, dim, scale, tok)
        got_a = exchange((s1, s2, s3))
        out[1], *g1s, keep_b, s1, s2, s3, tok = attention(1, dh[1], w_out, qkv[1], w_flat, dim, scale, tok)
        got_b = exchange((s1, s2, s3))
        dx_shard, tok = norm_shard(0, keep_a, got_a, x_saved, dh_shard[0], stats_one, g1, pos, tok)
        dx[0] = gather(dx_shard)
        grad_down, tok = weight_grad(act, grad_y, tok, 1024, 1024, 'dw2')
        grad_up, tok = weight_grad(n2, dpre, tok, 1024, 1024, 'dw1')
        dx_shard, tok = norm_shard(1, keep_b, got_b, x_saved, dh_shard[1], stats_one, g1, pos, tok)
        dx[1] = gather(dx_shard)
        grad_out_w, tok = weight_grad(out, dh, tok, 512, 1024, 'dwo')
        grad_qkv_w, grad_x, tok = qkv_grad(n1, [g0, g1s], heads, dim, dx[0], 2, tok)
        grad_x, tok = write_out(1, dx[1], grad_x, tok)
        return grad_x, grad_qkv_w.transpose(0, 2, 1, 3), grad_out_w.reshape(heads, dim, hid), grad_up, grad_down

    return jax.shard_map(local_backward, mesh=mesh, in_specs=in_specs, out_specs=out_specs, check_vma=False)
```
